128 devices in a mesh: space: 8 (over y_hi, x), dp: 16 (over y_lo, z, core).
Axes of the slice: x: 4, y: 4 (y_hi: 2, y_lo: 2; y = y_hi * 2 + y_lo), z: 4, core: 2. Of those that a mesh axis runs over, the one named last changes fastest.
Arguments:
- mixed_two: bfloat16 [16, 32, 180, 768], P('dp', 'space'), may hold values from -6 to 6
- input_two: bfloat16 [16, 32, 180, 768], P('dp', 'space'), may hold values from -6 to 6
- cotangent: bfloat16 [16, 32, 180, 768], P('dp', 'space'), may hold values from -6 to 6
- w_in_two: bfloat16 [3072, 768], replicated, may hold values from -0.21875 to 0.21875
- w_out_two: bfloat16 [3072, 768], replicated, may hold values from -0.109375 to 0.109375
- kernel_two: bfloat16 [9, 768], replicated, may hold values from -2 to 2
- mixed_one: bfloat16 [16, 32, 180, 768], P('dp', 'space'), may hold values from -6 to 6
- w_in_one: bfloat16 [3072, 768], replicated, may hold values from -0.21875 to 0.21875
- w_out_one: bfloat16 [3072, 768], replicated, may hold values from -0.109375 to 0.109375
- kernel_one: bfloat16 [9, 768], replicated, may hold values from -2 to 2
Outputs:
- input_grad: bfloat16 [16, 32, 180, 768], P('dp', 'space')
- grad_w_in: float32 [3072, 768], P('dp')
- grad_w_out: float32 [3072, 768], P('dp')
- grad_kernel: float32 [9, 768], replicated
The draws below stay inside these ranges and needn't reach their ends.
All inputs are finite; a program needn't handle non-finite values.
Results may differ from the reference program's by a relative error of at most 0.02.
Values may be sent and summed in bfloat16 or wider, within the bound.
A program may use at most 192 MiB of HBM per device.

```python
import math
import jax
import jax.numpy as jnp
from jax import lax

D = 768
FF = 3072
LON = 180
LAT = 32
BATCH = 16
TAPS = 9


def shard_levels(stream_key, extent, cuts, smallest, top_value):
    loudness = 1.0
    for dim, parts in cuts:
        steps = jax.random.uniform(jax.random.fold_in(jax.random.fold_in(stream_key, 6), dim), (parts,), jnp.float32, smallest / len(cuts), top_value / len(cuts))
        loudness = loudness * jnp.repeat(jnp.exp(steps), extent[dim] // parts).reshape((-1,) + (1,) * (len(extent) - 1 - dim))
    return loudness


def bell_draw(key, dims, width, limit, shards=(), held_as=jnp.bfloat16):
    drawn = jax.random.normal(key, dims, jnp.float32) * width
    if len(shards) > 0:
        drawn = shard_levels(key, dims, shards, -0.22, 0.18) * drawn
    return jnp.clip(drawn, min=-limit, max=limit).astype(held_as)


def setup_inputs(seed: int = 0) -> dict:
    seeds = jax.random.split(jax.random.key(seed), 11)
    mixed_two = bell_draw(seeds[0], (BATCH, LAT, LON, D), 1.0, 6.0, ((0, 16), (1, 8)))
    input_two = bell_draw(seeds[1], (BATCH, LAT, LON, D), 1.0, 6.0, ((0, 16), (1, 8)))
    cotangent = bell_draw(seeds[2], (BATCH, LAT, LON, D), 1.0, 6.0, ((0, 16), (1, 8)))
    w_in_two = bell_draw(seeds[3], (FF, D), D ** -0.5, 0.21875)
    w_out_two = bell_draw(seeds[4], (FF, D), FF ** -0.5, 0.109375)
    kernel_two = bell_draw(seeds[5], (TAPS, D), 0.35, 2.0)
    mixed_one = bell_draw(seeds[6], (BATCH, LAT, LON, D), 1.0, 6.0, ((0, 16), (1, 8)))
    w_in_one = bell_draw(seeds[7], (FF, D), D ** -0.5, 0.21875)
    w_out_one = bell_draw(seeds[8], (FF, D), FF ** -0.5, 0.109375)
    kernel_one = bell_draw(seeds[9], (TAPS, D), 0.35, 2.0)
    return {"mixed_two": mixed_two, "input_two": input_two, "cotangent": cotangent, "w_in_two": w_in_two, "w_out_two": w_out_two, "kernel_two": kernel_two, "mixed_one": mixed_one, "w_in_one": w_in_one, "w_out_one": w_out_one, "kernel_one": kernel_one}


GELU_C = math.sqrt(2.0 / math.pi)
CONTRACT_LAST = (((1,), (1,)), ((), ()))
CONTRACT_FIRST = (((0,), (0,)), ((), ()))

def gelu_parts(preact):
    tanh_arg = GELU_C * (preact + 0.044715 * preact * preact * preact)
    tanh_val = jnp.tanh(tanh_arg)
    activation = 0.5 * preact * (1.0 + tanh_val)
    gelu_slope = 0.5 * (1.0 + tanh_val) + 0.5 * preact * (1.0 - tanh_val * tanh_val) * GELU_C * (1.0 + 3.0 * 0.044715 * preact * preact)
    return (activation, gelu_slope)

def pad_rows(field):
    return jnp.pad(field, ((0, 0), (1, 1), (0, 0), (0, 0)))

def conv_back(padded, kernel, band_rows):
    kernel_f = kernel.astype(jnp.float32)
    result = jnp.zeros(padded[:, 1:1 + band_rows].shape, jnp.float32)
    for lat_off in range(3):
        for lon_off in range(3):
            window = padded[:, 2 - lat_off:2 - lat_off + band_rows].astype(jnp.float32)
            result = result + kernel_f[3 * lat_off + lon_off] * jnp.roll(window, lon_off - 1, axis=2)
    return result

def kernel_terms(padded_in, mix_grad, band_rows):
    grad_f = mix_grad.astype(jnp.float32)
    collected = []
    for lat_off in range(3):
        for lon_off in range(3):
            window = jnp.roll(padded_in[:, lat_off:lat_off + band_rows], 1 - lon_off, axis=2)
            collected.append(lax.optimization_barrier(jnp.sum(window.astype(jnp.float32) * grad_f, axis=(0, 1, 2))))
    return jnp.stack(collected)

def reference(mixed_two, input_two, cotangent, w_in_two, w_out_two, kernel_two, mixed_one, w_in_one, w_out_one, kernel_one):

    def sample_pass(items):
        mixed_late, input_late, cot_late, mixed_early = [item[None] for item in items]
        shape4 = mixed_late.shape
        band_rows = shape4[1]
        channels = shape4[3]
        mixed_flat = mixed_late.reshape(-1, channels)
        cot_flat = cot_late.reshape(-1, channels)
        preact = lax.dot_general(mixed_flat, w_in_two, CONTRACT_LAST, preferred_element_type=jnp.float32)
        activation, gelu_slope = gelu_parts(preact)
        activation = activation.astype(jnp.bfloat16)
        hidden_grad = lax.dot_general(cot_flat, w_out_two, CONTRACT_LAST, preferred_element_type=jnp.float32)
        pre_grad = (hidden_grad * gelu_slope).astype(jnp.bfloat16)
        mix_grad = jnp.dot(pre_grad, w_in_two, preferred_element_type=jnp.float32).astype(jnp.bfloat16).reshape(shape4)
        out_term = lax.dot_general(activation, cot_flat, CONTRACT_FIRST, preferred_element_type=jnp.float32)
        in_term = lax.dot_general(pre_grad, mixed_flat, CONTRACT_FIRST, preferred_element_type=jnp.float32)
        taps_term = kernel_terms(pad_rows(input_late), mix_grad, band_rows)
        grad_two = (cot_late.astype(jnp.float32) + conv_back(pad_rows(mix_grad), kernel_two, band_rows)).astype(jnp.bfloat16)
        preact_early = lax.dot_general(mixed_early.reshape(-1, channels), w_in_one, CONTRACT_LAST, preferred_element_type=jnp.float32)
        unused_act, slope_early = gelu_parts(preact_early)
        hidden_early = lax.dot_general(grad_two.reshape(-1, channels), w_out_one, CONTRACT_LAST, preferred_element_type=jnp.float32)
        pre_early = (hidden_early * slope_early).astype(jnp.bfloat16)
        mix_early = jnp.dot(pre_early, w_in_one, preferred_element_type=jnp.float32).astype(jnp.bfloat16).reshape(shape4)
        grad_one = (grad_two.astype(jnp.float32) + conv_back(pad_rows(mix_early), kernel_one, band_rows)).astype(jnp.bfloat16)
        return (grad_one[0], in_term, out_term, taps_term)
    grad_one, in_terms, out_terms, tap_terms = lax.map(sample_pass, (mixed_two, input_two, cotangent, mixed_one))
    grad_w_in = lax.optimization_barrier(jnp.sum(in_terms, axis=0)) / BATCH
    grad_w_out = lax.optimization_barrier(jnp.sum(out_terms, axis=0)) / BATCH
    grad_kernel = lax.optimization_barrier(jnp.sum(tap_terms, axis=0)) / BATCH
    return (grad_one, grad_w_in, grad_w_out, grad_kernel)
```

```python
import math

import jax
import jax.numpy as jnp
from jax import lax
from jax.experimental import pallas as pl
from jax.experimental.pallas import tpu as pltpu
from jax.sharding import Mesh
from jax.sharding import PartitionSpec as P

AXES = ("space_0", "space_1", "dp_0", "dp_1", "dp_2")
SPACE = ("space_0", "space_1")
DP = ("dp_0", "dp_1", "dp_2")
MESH = pl.DeviceIdType.MESH
GELU_C = math.sqrt(2.0 / math.pi)
GELU_A = GELU_C * 0.044715
LAST = (((1,), (1,)), ((), ()))
F32 = jnp.float32
BF16 = jnp.bfloat16

D = 768
FF = 3072
LON = 180
PAD = 192
TOK = 4 * PAD
HALF = 2 * PAD
BLK = 384
STEPS = FF // BLK
SUB = 48
GROUPS = 6
LANES = 128
ORDER = (0, 3, 1, 2)
CYCLE = (5, 3, 1, 4, 2, 0)
PERM = tuple(tuple(CYCLE[(g + i) % 6] for i in range(6)) for g in range(GROUPS))


def place_of(group, bits):
    where = 0
    for i, bit in enumerate(PERM[group]):
        where = where + bits[bit] * (1 << (5 - i))
    return where


def gelu_all(v):
    v2 = v * v
    t = jnp.tanh(v * (GELU_C + GELU_A * v2))
    q = 0.5 + 0.5 * t
    slope = q + (v * (1.0 - t * t)) * (0.5 * GELU_C + (1.5 * GELU_A) * v2)
    return v * q, slope


def body(
    mx2_h, in2_h, ct_h, win2_h, wout2_h, k2_h, mx1_h, win1_h, wout1_h, k1_h,
    out_h, gin_h, gout_h, gk_h,
    mx2, ct, mx1, in2, inh, win2, wout2, win1, kt2, kt1,
    pre, slopes, mge, g2, outv, ginv, goutv, kg, kgr,
    stage, d2d, buf, rcv, ag,
    load_sem, d2d_s, d2d_r, rs_s, rs_r, ag_s, ag_r, kg_s, kg_r, halo_s, halo_r, out_sem,
):
    yhi = lax.axis_index("space_0")
    x = lax.axis_index("space_1")
    ylo = lax.axis_index("dp_0")
    z = lax.axis_index("dp_1")
    core = lax.axis_index("dp_2")
    gx1, gx0 = x // 2, (x // 2 + x) % 2
    gz1, gz0 = z // 2, (z // 2 + z) % 2
    near = {
        5: (yhi, 2 * (x // 2) + 1 - x % 2, ylo, z, core),
        4: (yhi, 3 - x, ylo, z, core),
        3: (yhi, x, 1 - ylo, z, core),
        2: (1 - yhi, x, 1 - ylo, z, core),
        1: (yhi, x, ylo, 2 * (z // 2) + 1 - z % 2, core),
        0: (yhi, x, ylo, 3 - z, core),
        "c": (yhi, x, ylo, z, 1 - core),
        "yy": (1 - yhi, x, ylo, z, core),
        "up": ((yhi + x // 3) % 2, (x + 1) % 4, ylo, z, core),
        "down": ((yhi + (3 - x) // 3) % 2, (x + 3) % 4, ylo, z, core),
    }
    first_band = (yhi * 4 + x) == 0
    last_band = (yhi * 4 + x) == 7

    def block_of(s):
        r = 7 - s
        a1, a0, c = r // 4, (r // 2) % 2, r % 2
        z1, z0 = (gz1 + a1) % 2, (gz0 + a0) % 2
        zz = 2 * z1 + (z1 + z0) % 2
        yy = (ylo + c) % 2
        rows = pl.multiple_of((yy * 4 + zz) * BLK, BLK)
        return rows, a1, a0, c

    whole = [
        pltpu.make_async_copy(a, b, load_sem.at[i])
        for i, (a, b) in enumerate(
            ((mx2_h, mx2), (ct_h, ct), (in2_h, in2), (mx1_h, mx1), (win1_h, win1), (k2_h, kt2), (k1_h, kt1))
        )
    ]
    late = pltpu.make_async_copy(wout1_h, wout2, load_sem.at[7])

    def weight_copy(s, which):
        rows = pl.ds(block_of(s)[0], BLK)
        src, dst = ((win2_h, win2), (wout2_h, wout2))[which]
        return pltpu.make_async_copy(src.at[rows], dst.at[rows], load_sem.at[8 + 8 * which + s])

    whole[0].start()
    weight_copy(0, 0).start()
    whole[1].start()
    weight_copy(0, 1).start()

    @pl.loop(1, STEPS)
    def _(s):
        weight_copy(s, 0).start()
        weight_copy(s, 1).start()

    for i in (2, 3, 4, 5, 6):
        whole[i].start()

    barrier = pltpu.get_barrier_semaphore()
    for who in near.values():
        pl.semaphore_signal(barrier, inc=1, device_id=who, device_id_type=MESH)
    pl.semaphore_wait(barrier, len(near))

    def remote(src, dst, ssem, rsem, who):
        return pltpu.make_async_remote_copy(
            src_ref=src, dst_ref=dst, send_sem=ssem, recv_sem=rsem, device_id=near[who], device_id_type=MESH
        )

    def core_copy(s):
        return remote(stage.at[s % 2, 1], d2d.at[s], d2d_s.at[s], d2d_r.at[s], "c")

    def core_add(s):
        rows, a1, a0, c = block_of(s)
        copy = core_copy(s)
        copy.wait_recv()

        @pl.loop(0, 8)
        def _(mq):
            m, q1, q0 = mq // 4, (mq // 2) % 2, mq % 2
            bits = (a1, a0, m, (c + m) % 2, q1, q0)
            for g in range(GROUPS):
                total = stage[s % 2, 0, mq, g].astype(F32) + d2d[s, mq, g].astype(F32)
                buf[g, place_of(g, bits)] = total.astype(BF16)

        copy.wait_send()

    def rs_copy(i, g):
        half = pl.ds(1 << (5 - i), 1 << (5 - i))
        return remote(buf.at[g, half], rcv.at[g, half], rs_s.at[i, g], rs_r.at[i, g], PERM[g][i])

    def rs_send(i):
        for g in range(GROUPS):
            rs_copy(i, g).start()

    def rs_add(i):
        count = 1 << (5 - i)
        for g in range(GROUPS):
            rs_copy(i, g).wait_recv()

        @pl.loop(0, count)
        def _(n):
            for g in range(GROUPS):
                buf[g, n] = (buf[g, n].astype(F32) + rcv[g, count + n].astype(F32)).astype(BF16)

    ag_list = [
        (0, (0, 0, 0), (0, 0, 1), "yy"),
        (1, (1, 0, 0), (1, 0, 1), "yy"),
        (2, (0, 0), (0, 1), 5),
        (3, (1, 0), (1, 2), 4),
        (4, (0, 0), (0, 2), 4),
        (5, (0, 1), (0, 3), 4),
        (6, (1, 0), (1, 1), 5),
        (7, (1, 2), (1, 3), 5),
    ]

    def ag_copy(n):
        _, src, dst, who = ag_list[n]
        return remote(ag.at[src], ag.at[dst], ag_s.at[n], ag_r.at[n], who)

    kg_bits = ("c", 5, 3, 1, 4, 2, 0)

    def kg_copy(t):
        return remote(kg.at[t], kgr.at[t], kg_s.at[t], kg_r.at[t], kg_bits[t])

    def kg_next(t):
        kg_copy(t).wait_recv()
        kg[t + 1] = kg[t] + kgr[t]
        if t + 1 < len(kg_bits):
            kg_copy(t + 1).start()

    halos = [
        remote(in2.at[0], inh.at[1], halo_s.at[0], halo_r.at[0], "down"),
        remote(in2.at[3], inh.at[0], halo_s.at[1], halo_r.at[1], "up"),
        remote(mge.at[1], mge.at[5], halo_s.at[2], halo_r.at[2], "down"),
        remote(mge.at[4], mge.at[0], halo_s.at[3], halo_r.at[3], "up"),
        remote(mge.at[7], mge.at[11], halo_s.at[4], halo_r.at[4], "down"),
        remote(mge.at[10], mge.at[6], halo_s.at[5], halo_r.at[5], "up"),
    ]

    whole[0].wait()
    whole[1].wait()

    @pl.loop(0, STEPS)
    def _(s):
        rows = pl.ds(block_of(s)[0], BLK)
        weight_copy(s, 0).wait()
        weight_copy(s, 1).wait()
        p = lax.dot_general(win2[rows, :], mx2[...], LAST, preferred_element_type=F32)
        h = lax.dot_general(wout2[rows, :], ct[...], LAST, preferred_element_type=F32)
        act, slope = gelu_all(p)
        pg = (h * slope).astype(BF16)
        terms = (
            jnp.dot(pg, mx2[...], preferred_element_type=F32).astype(BF16),
            jnp.dot(act.astype(BF16), ct[...], preferred_element_type=F32).astype(BF16),
        )
        pre[:, rows] = pg.T
        for m in range(2):
            mm = (m + yhi) % 2
            for half in range(2):
                slot = (half + core) % 2
                for q in range(4):
                    qq = ((q // 2 + gx1) % 2) * 2 + (q % 2 + gx0) % 2
                    lo = half * PAD + q * SUB
                    for g in range(GROUPS):
                        stage[s % 2, slot, mm * 4 + qq, g] = terms[m][lo : lo + SUB, g * LANES : (g + 1) * LANES]
        core_copy(s).start()

        @pl.when(s > 0)
        def _():
            core_add(s - 1)

    late.start()
    for i in (2, 3, 4, 5, 6):
        whole[i].wait()
    halos[0].start()
    halos[1].start()

    def mixed_back(src, w, top, base, pair):
        @pl.loop(0, 3)
        def _(nb):
            cols = pl.ds(pl.multiple_of(nb * 256, 256), 256)
            r = jnp.dot(src[top : top + HALF, :], w[:, cols], preferred_element_type=F32).astype(BF16)
            mge[base + pair[0], :, cols] = r[:PAD]
            mge[base + pair[1], :, cols] = r[PAD:]

    mixed_back(pre, win2, 0, 0, (1, 4))
    halos[2].start()
    halos[3].start()
    core_add(STEPS - 1)
    rs_send(0)
    mixed_back(pre, win2, HALF, 0, (2, 3))

    @pl.loop(0, STEPS)
    def _(s):
        rows = pl.ds(pl.multiple_of(s * BLK, BLK), BLK)
        p = lax.dot_general(mx1[...], win1[rows, :], LAST, preferred_element_type=F32)
        slopes[:, rows] = gelu_all(p)[1].astype(BF16)

    def halo_wait(pair, low, high):
        halos[pair].wait_recv()
        halos[pair + 1].wait_recv()

        @pl.when(first_band)
        def _():
            low[...] = jnp.zeros((PAD, D), BF16)

        @pl.when(last_band)
        def _():
            high[...] = jnp.zeros((PAD, D), BF16)

    at_row = lax.broadcasted_iota(jnp.int32, (PAD, LANES), 0)

    def back(v):
        return jnp.where(at_row == LON - 1, v[0:1], pltpu.roll(v, PAD - 1, 0))

    def ahead(v):
        return jnp.where(at_row == 0, v[LON - 1 : LON], pltpu.roll(v, 1, 0))

    halo_wait(0, inh.at[0], inh.at[1])
    halo_wait(2, mge.at[0], mge.at[5])

    kg[0, 8:16] = jnp.zeros((8, D), F32)

    @pl.loop(0, 6)
    def _(lb):
        cols = pl.ds(pl.multiple_of(lb * LANES, LANES), LANES)
        totals = [jnp.zeros((8, LANES), F32) for _ in range(9)]
        for i in range(4):
            v = jnp.where(at_row < LON, mge[i + 1, :, cols].astype(F32), 0.0)
            rolled = (back(v), v, ahead(v))
            for a in range(3):
                e = i + a - 1
                field = inh[0, :, cols] if e < 0 else inh[1, :, cols] if e > 3 else in2[e, :, cols]
                field = field.astype(F32)
                for b in range(3):
                    totals[3 * a + b] += (field * rolled[b]).reshape(PAD // 8, 8, LANES).sum(0)
        for n in range(9):
            kg[0, n : n + 1, cols] = totals[n].sum(0, keepdims=True)

    kg_copy(0).start()

    def mix_transposed(base, kt, get, put):
        @pl.loop(0, 6)
        def _(lb):
            cols = pl.ds(pl.multiple_of(lb * LANES, LANES), LANES)
            taps = kt[:, cols].astype(F32)
            for i in range(4):
                sums = [jnp.zeros((PAD, LANES), F32) for _ in range(3)]
                for a in range(3):
                    v = mge[base + i - a + 2, :, cols].astype(F32)
                    for b in range(3):
                        sums[b] += taps[3 * a + b : 3 * a + b + 1] * v
                put(i, cols, get(i, cols) + sums[1] + back(sums[0]) + ahead(sums[2]))

    def ct_row(i, cols):
        at = ORDER.index(i) * PAD
        return ct[at : at + PAD, cols].astype(F32)

    def g2_row(i, cols):
        at = ORDER.index(i) * PAD
        return g2[at : at + PAD, cols].astype(F32)

    def put_g2(i, cols, v):
        at = ORDER.index(i) * PAD
        g2[at : at + PAD, cols] = jnp.where(at_row < LON, v, 0.0).astype(BF16)

    def put_out(i, cols, v):
        outv[i, :, cols] = v[:LON].astype(BF16)

    mix_transposed(0, kt2, ct_row, put_g2)
    rs_add(0)
    rs_send(1)
    kg_next(0)
    late.wait()

    def hidden_back(top):
        @pl.loop(0, STEPS)
        def _(s):
            rows = pl.ds(pl.multiple_of(s * BLK, BLK), BLK)
            h = lax.dot_general(g2[top : top + HALF, :], wout2[rows, :], LAST, preferred_element_type=F32)
            pre[top : top + HALF, rows] = (h * slopes[top : top + HALF, rows].astype(F32)).astype(BF16)

    hidden_back(0)
    rs_add(1)
    rs_send(2)
    kg_next(1)
    mixed_back(pre, win1, 0, 6, (1, 4))
    halos[4].start()
    halos[5].start()
    rs_add(2)
    rs_send(3)
    kg_next(2)
    hidden_back(HALF)
    rs_add(3)
    rs_send(4)
    kg_next(3)
    mixed_back(pre, win1, HALF, 6, (2, 3))
    rs_add(4)
    rs_send(5)
    kg_next(4)
    halo_wait(4, mge.at[6], mge.at[11])
    mix_transposed(6, kt1, g2_row, put_out)
    out_copy = pltpu.make_async_copy(outv, out_h.at[0], out_sem.at[0])
    out_copy.start()
    rs_add(5)
    kg_next(5)
    for g in range(GROUPS):
        ag[g // 3, 0, 0, g % 3] = buf[g, 0]
    ag_copy(0).start()
    ag_copy(1).start()
    kg_next(6)
    ag_copy(0).wait_recv()
    ag_copy(1).wait_recv()
    ag_copy(2).start()
    ag_copy(3).start()
    ag_copy(2).wait_recv()
    ag_copy(3).wait_recv()
    for n in (4, 5, 6, 7):
        ag_copy(n).start()
    for n in (4, 5, 6, 7):
        ag_copy(n).wait_recv()

    scale = 1.0 / 16.0
    for m, dst in ((0, ginv), (1, goutv)):
        mm = (m + yhi) % 2
        for q in range(4):
            qq = ((q // 2 + gx1) % 2) * 2 + (q % 2 + gx0) % 2
            for g in range(GROUPS):
                dst[q * SUB : (q + 1) * SUB, g * LANES : (g + 1) * LANES] = ag[g // 3, qq, mm, g % 3].astype(F32) * scale
    kg[8] = kg[7] * scale
    outs = [
        pltpu.make_async_copy(ginv, gin_h, out_sem.at[1]),
        pltpu.make_async_copy(goutv, gout_h, out_sem.at[2]),
        pltpu.make_async_copy(kg.at[8], gk_h, out_sem.at[3]),
    ]
    for o in outs:
        o.start()
    for n in range(6):
        halos[n].wait_send()
    for i in range(6):
        for g in range(GROUPS):
            rs_copy(i, g).wait_send()
    for n in range(8):
        ag_copy(n).wait_send()
    for t in range(7):
        kg_copy(t).wait_send()
    out_copy.wait()
    for o in outs:
        o.wait()


def in_rows(a):
    return jnp.pad(a[0], ((0, 0), (0, PAD - LON), (0, 0)))


def in_order(a):
    rows = in_rows(a)
    return jnp.concatenate([rows[i] for i in ORDER], axis=0)


def step(mixed_two, input_two, cotangent, w_in_two, w_out_two, kernel_two, mixed_one, w_in_one, w_out_one, kernel_one):
    dma = pltpu.SemaphoreType.DMA
    vmem = pltpu.VMEM
    tokens = (TOK, D)
    taps = lambda k: jnp.pad(k, ((0, 7), (0, 0)))
    out, gin, gout, gk = pl.pallas_call(
        body,
        out_shape=(
            jax.ShapeDtypeStruct((1, 4, LON, D), BF16),
            jax.ShapeDtypeStruct((PAD, D), F32),
            jax.ShapeDtypeStruct((PAD, D), F32),
            jax.ShapeDtypeStruct((16, D), F32),
        ),
        in_specs=[pl.BlockSpec(memory_space=pl.ANY)] * 10,
        out_specs=[pl.BlockSpec(memory_space=pl.ANY)] * 4,
        scratch_shapes=[
            vmem(tokens, BF16), vmem(tokens, BF16), vmem(tokens, BF16),
            vmem((4, PAD, D), BF16), vmem((2, PAD, D), BF16),
            vmem((FF, D), BF16), vmem((FF, D), BF16), vmem((FF, D), BF16),
            vmem((16, D), BF16), vmem((16, D), BF16),
            vmem((TOK, FF), BF16), vmem((TOK, FF), BF16),
            vmem((12, PAD, D), BF16), vmem(tokens, BF16), vmem((4, LON, D), BF16),
            vmem((PAD, D), F32), vmem((PAD, D), F32),
            vmem((9, 16, D), F32), vmem((7, 16, D), F32),
            vmem((2, 2, 8, GROUPS, SUB, LANES), BF16),
            vmem((STEPS, 8, GROUPS, SUB, LANES), BF16),
            vmem((GROUPS, 64, SUB, LANES), BF16),
            vmem((GROUPS, 64, SUB, LANES), BF16),
            vmem((2, 4, 2, 3, SUB, LANES), BF16),
            dma((24,)), dma((STEPS,)), dma((STEPS,)), dma((6, GROUPS)), dma((6, GROUPS)),
            dma((8,)), dma((8,)), dma((7,)), dma((7,)), dma((6,)), dma((6,)), dma((4,)),
        ],
        compiler_params=pltpu.CompilerParams(
            collective_id=0, has_side_effects=True, vmem_limit_bytes=67000000
        ),
    )(
        in_order(mixed_two), in_rows(input_two), in_order(cotangent), w_in_two, w_out_two, taps(kernel_two),
        in_order(mixed_one), w_in_one, w_out_one, taps(kernel_one),
    )
    return out, gin, gout, gk[:9]


def solution(mesh):
    finer = Mesh(mesh.devices.reshape(2, 4, 2, 4, 2), AXES)
    grid = P(DP, SPACE, None, None)
    return jax.shard_map(
        step,
        mesh=finer,
        in_specs=(grid, grid, grid, P(), P(), P(), grid, P(), P(), P()),
        out_specs=(grid, P(DP, None), P(DP, None), P()),
        check_vma=False,
    )
```

```python
import math

import jax
import jax.numpy as jnp
from jax import lax
from jax.experimental import pallas as pl
from jax.experimental.pallas import tpu as pltpu
from jax.sharding import Mesh
from jax.sharding import PartitionSpec as P

AXES = ("space_0", "space_1", "dp_0", "dp_1", "dp_2")
SPACE = ("space_0", "space_1")
DP = ("dp_0", "dp_1", "dp_2")
MESH = pl.DeviceIdType.MESH
GELU_C = math.sqrt(2.0 / math.pi)
GELU_A = GELU_C * 0.044715
LAST = (((1,), (1,)), ((), ()))
F32 = jnp.float32
BF16 = jnp.bfloat16

D = 768
FF = 3072
LON = 180
PAD = 192
TOK = 4 * PAD
HALF = 2 * PAD
BLK = 384
STEPS = FF // BLK
SUB = 48
TAPS = 9
GROUPS = 6
LANES = 128
VMEM_LIMIT = 44 << 20
SLOTS = 4
ORDER = (0, 3, 1, 2)
PERM = (
    (5, 3, 1, 2, 0, 4),
    (3, 5, 0, 1, 2, 4),
    (1, 4, 3, 0, 2, 5),
    (4, 1, 2, 3, 0, 5),
    (2, 0, 5, 1, 3, 4),
    (0, 2, 4, 3, 1, 5),
)


def place_of(group, bits):
    where = 0
    for i, bit in enumerate(PERM[group]):
        where = where + bits[bit] * (1 << (5 - i))
    return where


def gelu_all(v):
    v2 = v * v
    t = jnp.tanh(v * (GELU_C + GELU_A * v2))
    q = 0.5 + 0.5 * t
    slope = q + (v * (1.0 - t * t)) * (0.5 * GELU_C + (1.5 * GELU_A) * v2)
    return v * q, slope


def body(
    mx2, in2, ct, win2_h, wout2_h, kt2, mx1, win1_h, wout1_h, kt1,
    outv, ginv, goutv, gkv,
    inh, win2, wout2, win1,
    pre, mge, g2, kg, kgr,
    stage, d2d, buf, rcv, ag,
    load_sem, d2d_s, d2d_r, rs_s, rs_r, ag_s, ag_r, kg_s, kg_r, halo_s, halo_r,
):
    yhi = lax.axis_index("space_0")
    x = lax.axis_index("space_1")
    ylo = lax.axis_index("dp_0")
    z = lax.axis_index("dp_1")
    core = lax.axis_index("dp_2")
    gx1, gx0 = x // 2, (x // 2 + x) % 2
    gz1, gz0 = z // 2, (z // 2 + z) % 2
    near = {
        5: (yhi, 2 * (x // 2) + 1 - x % 2, ylo, z, core),
        4: (yhi, 3 - x, ylo, z, core),
        3: (yhi, x, 1 - ylo, z, core),
        2: (1 - yhi, x, 1 - ylo, z, core),
        1: (yhi, x, ylo, 2 * (z // 2) + 1 - z % 2, core),
        0: (yhi, x, ylo, 3 - z, core),
        "c": (yhi, x, ylo, z, 1 - core),
        "yy": (1 - yhi, x, ylo, z, core),
        "up": ((yhi + x // 3) % 2, (x + 1) % 4, ylo, z, core),
        "down": ((yhi + (3 - x) // 3) % 2, (x + 3) % 4, ylo, z, core),
    }
    first_band = (yhi * 4 + x) == 0
    last_band = (yhi * 4 + x) == 7

    def block_of(s):
        r = 7 - s
        a1, a0, c = r // 4, (r // 2) % 2, r % 2
        z1, z0 = (gz1 + a1) % 2, (gz0 + a0) % 2
        zz = 2 * z1 + (z1 + z0) % 2
        yy = (ylo + c) % 2
        rows = pl.multiple_of((yy * 4 + zz) * BLK, BLK)
        return rows, a1, a0, c

    other = pltpu.make_async_copy(win1_h, win1, load_sem.at[16])
    late = pltpu.make_async_copy(wout1_h, wout2, load_sem.at[17])

    def weight_copy(s, which):
        rows = pl.ds(block_of(s)[0], BLK)
        src, dst = ((win2_h, win2), (wout2_h, wout2))[which]
        return pltpu.make_async_copy(src.at[rows], dst.at[rows], load_sem.at[8 * which + s])

    @pl.loop(0, STEPS)
    def _(s):
        weight_copy(s, 0).start()
        weight_copy(s, 1).start()

    other.start()

    barrier = pltpu.get_barrier_semaphore()
    for who in near.values():
        pl.semaphore_signal(barrier, inc=1, device_id=who, device_id_type=MESH)
    pl.semaphore_wait(barrier, len(near))

    def remote(src, dst, ssem, rsem, who):
        return pltpu.make_async_remote_copy(
            src_ref=src, dst_ref=dst, send_sem=ssem, recv_sem=rsem, device_id=near[who], device_id_type=MESH
        )

    def core_copy(s):
        return remote(stage.at[s % 2, 1], d2d.at[s % SLOTS], d2d_s.at[s], d2d_r.at[s], "c")

    def core_add(s):
        rows, a1, a0, c = block_of(s)
        copy = core_copy(s)
        copy.wait_recv()
        for mq in range(8):
            m, q1, q0 = mq // 4, (mq // 2) % 2, mq % 2
            for g in range(GROUPS):
                at = place_of(g, (a1, a0, m, (c + m) % 2, q1, q0))
                buf[g, at] = stage[s % 2, 0, mq, g] + d2d[s % SLOTS, mq, g]
        copy.wait_send()
        first_sends(a1, a0, c)

    def pair_copy(g, a1, a0, c, m, u):
        x1, x0 = (0, u) if PERM[g][5] == 4 else (u, 0)
        at = pl.ds(place_of(g, (a1, a0, m, (c + m) % 2, x1, x0)), 2)
        return remote(buf.at[g, at], rcv.at[g, at], rs_s.at[0, g], rs_r.at[0, g], PERM[g][0])

    def first_sends(a1, a0, c):
        for g in range(GROUPS):
            bit = PERM[g][0]
            if bit in (4, 5):
                for m in range(2):
                    pair_copy(g, a1, a0, c, m, 1).start()
            elif bit in (2, 3):
                for u in range(2):
                    pair_copy(g, a1, a0, c, 1 if bit == 2 else 1 - c, u).start()

        for bit, flag in ((1, a0), (0, a1)):
            g = [p[0] for p in PERM].index(bit)
            if flag == 1:
                for m in range(2):
                    for u in range(2):
                        pair_copy(g, a1, a0, c, m, u).start()

    def rs_copy(i, g):
        half = pl.ds(1 << (5 - i), 1 << (5 - i))
        return remote(buf.at[g, half], rcv.at[g, half], rs_s.at[i, g], rs_r.at[i, g], PERM[g][i])

    def rs_send(i):
        for g in range(GROUPS):
            rs_copy(i, g).start()

    def rs_add(i):
        count = 1 << (5 - i)
        for g in range(GROUPS):
            rs_copy(i, g).wait_recv()

        @pl.loop(0, count)
        def _(n):
            for g in range(GROUPS):
                buf[g, n] = buf[g, n] + rcv[g, count + n]

    ag_list = [
        (0, (0, 0, 0), (0, 0, 1), "yy"),
        (1, (1, 0, 0), (1, 0, 1), "yy"),
        (2, (0, 0), (0, 1), 5),
        (3, (1, 0), (1, 2), 4),
        (4, (0, 0), (0, 2), 4),
        (5, (0, 1), (0, 3), 4),
        (6, (1, 0), (1, 1), 5),
        (7, (1, 2), (1, 3), 5),
    ]

    def ag_copy(n):
        _, src, dst, who = ag_list[n]
        return remote(ag.at[src], ag.at[dst], ag_s.at[n], ag_r.at[n], who)

    kg_bits = ("c", 5, 3, 1, 4, 2, 0)

    def kg_copy(t):
        return remote(kg.at[t], kgr.at[t], kg_s.at[t], kg_r.at[t], kg_bits[t])

    def kg_next(t):
        kg_copy(t).wait_recv()
        kg[t + 1] = kg[t] + kgr[t]
        if t + 1 < len(kg_bits):
            kg_copy(t + 1).start()

    halos = [
        remote(in2.at[0], inh.at[1], halo_s.at[0], halo_r.at[0], "down"),
        remote(in2.at[3], inh.at[0], halo_s.at[1], halo_r.at[1], "up"),
        remote(mge.at[1], mge.at[5], halo_s.at[2], halo_r.at[2], "down"),
        remote(mge.at[4], mge.at[0], halo_s.at[3], halo_r.at[3], "up"),
        remote(mge.at[7], mge.at[11], halo_s.at[4], halo_r.at[4], "down"),
        remote(mge.at[10], mge.at[6], halo_s.at[5], halo_r.at[5], "up"),
    ]

    halos[0].start()
    halos[1].start()

    for s in range(STEPS):
        rows = pl.ds(block_of(s)[0], BLK)
        weight_copy(s, 0).wait()
        weight_copy(s, 1).wait()
        p = lax.dot_general(win2[rows, :], mx2[...], LAST, preferred_element_type=F32)
        h = lax.dot_general(wout2[rows, :], ct[...], LAST, preferred_element_type=F32)
        act, slope = gelu_all(p)
        pg = (h * slope).astype(BF16)
        terms = (
            jnp.dot(pg, mx2[...], preferred_element_type=F32).astype(BF16),
            jnp.dot(act.astype(BF16), ct[...], preferred_element_type=F32).astype(BF16),
        )
        pre[:, rows] = pg.T
        for m in range(2):
            mm = (m + yhi) % 2
            for half in range(2):
                slot = (half + core) % 2
                for q in range(4):
                    qq = ((q // 2 + gx1) % 2) * 2 + (q % 2 + gx0) % 2
                    lo = half * PAD + q * SUB
                    for g in range(GROUPS):
                        stage[s % 2, slot, mm * 4 + qq, g] = terms[m][lo : lo + SUB, g * LANES : (g + 1) * LANES]
        core_copy(s).start()
        if s > 0:
            core_add(s - 1)

    late.start()

    def mixed_back(src, w, top, base, pair):
        @pl.loop(0, 3)
        def _(nb):
            cols = pl.ds(pl.multiple_of(nb * 256, 256), 256)
            r = jnp.dot(src[top : top + HALF, :], w[:, cols], preferred_element_type=F32).astype(BF16)
            mge[base + pair[0], :, cols] = r[:PAD]
            mge[base + pair[1], :, cols] = r[PAD:]

    def halo_wait(pair, low, high):
        halos[pair].wait_recv()
        halos[pair + 1].wait_recv()

        @pl.when(first_band)
        def _():
            low[...] = jnp.zeros((PAD, D), BF16)

        @pl.when(last_band)
        def _():
            high[...] = jnp.zeros((PAD, D), BF16)

    at_row = lax.broadcasted_iota(jnp.int32, (PAD, LANES), 0)

    def back(v):
        return jnp.where(at_row == LON - 1, v[0:1], pltpu.roll(v, PAD - 1, 0))

    def ahead(v):
        return jnp.where(at_row == 0, v[LON - 1 : LON], pltpu.roll(v, 1, 0))

    def kernel_gradient():
        kg[0, 8:16] = jnp.zeros((8, D), F32)

        @pl.loop(0, 6)
        def _(lb):
            cols = pl.ds(pl.multiple_of(lb * LANES, LANES), LANES)
            totals = [jnp.zeros((1, LANES), F32) for _ in range(9)]
            for i in range(4):
                v = jnp.where(at_row < LON, mge[i + 1, :, cols].astype(F32), 0.0)
                rolled = (back(v).astype(BF16), v.astype(BF16), ahead(v).astype(BF16))
                for a in range(3):
                    e = i + a - 1
                    field = inh[0, :, cols] if e < 0 else inh[1, :, cols] if e > 3 else in2[e, :, cols]
                    for b in range(3):
                        term = (field * rolled[b]).reshape(PAD // 16, 16, LANES)
                        part = term[0]
                        for n in range(1, PAD // 16):
                            part = part + term[n]
                        totals[3 * a + b] += part.astype(F32).sum(0, keepdims=True)
            for n in range(9):
                kg[0, n : n + 1, cols] = totals[n]

    def mix_transposed(base, kt, get, put, rows):
        @pl.loop(0, 6)
        def _(lb):
            cols = pl.ds(pl.multiple_of(lb * LANES, LANES), LANES)
            taps = kt[:, cols]
            for i in rows:
                sums = [None] * 3
                for a in range(3):
                    v = mge[base + i - a + 2, :, cols]
                    for b in range(3):
                        term = taps[3 * a + b : 3 * a + b + 1] * v
                        sums[b] = term if a == 0 else sums[b] + term
                sums = [t.astype(F32) for t in sums]
                put(i, cols, get(i, cols) + sums[1] + back(sums[0]) + ahead(sums[2]))

    def ct_row(i, cols):
        at = ORDER.index(i) * PAD
        return ct[at : at + PAD, cols].astype(F32)

    def g2_row(i, cols):
        at = ORDER.index(i) * PAD
        return g2[at : at + PAD, cols].astype(F32)

    def put_g2(i, cols, v):
        at = ORDER.index(i) * PAD
        g2[at : at + PAD, cols] = jnp.where(at_row < LON, v, 0.0).astype(BF16)

    def put_out(i, cols, v):
        outv[0, i, :, cols] = v[:LON].astype(BF16)

    def slopes_one(first, count):
        @pl.loop(first, first + count)
        def _(s):
            rows = pl.ds(pl.multiple_of(s * BLK, BLK), BLK)
            p = lax.dot_general(mx1[...], win1[rows, :], LAST, preferred_element_type=F32)
            pre[:, rows] = gelu_all(p)[1].astype(BF16)

    def hidden_back(top, first, count):
        @pl.loop(first, first + count)
        def _(s):
            rows = pl.ds(pl.multiple_of(s * BLK, BLK), BLK)
            h = lax.dot_general(g2[top : top + HALF, :], wout2[rows, :], LAST, preferred_element_type=F32)
            pre[top : top + HALF, rows] = (h * pre[top : top + HALF, rows].astype(F32)).astype(BF16)

    core_add(STEPS - 1)
    mixed_back(pre, win2, 0, 0, (1, 4))
    rs_add(0)
    rs_send(1)
    halos[2].start()
    halos[3].start()
    mixed_back(pre, win2, HALF, 0, (2, 3))
    other.wait()
    slopes_one(0, 4)
    mix_transposed(0, kt2, ct_row, put_g2, (1, 2))
    rs_add(1)
    rs_send(2)
    slopes_one(4, 4)
    halo_wait(0, inh.at[0], inh.at[1])
    kernel_gradient()
    kg_copy(0).start()
    rs_add(2)
    rs_send(3)
    halo_wait(2, mge.at[0], mge.at[5])
    mix_transposed(0, kt2, ct_row, put_g2, (0, 3))
    late.wait()
    kg_next(0)
    hidden_back(0, 0, 4)
    rs_add(3)
    rs_send(4)
    kg_next(1)
    hidden_back(0, 4, 4)
    rs_add(4)
    rs_send(5)
    kg_next(2)
    mixed_back(pre, win1, 0, 6, (1, 4))
    halos[4].start()
    halos[5].start()
    rs_add(5)
    for g in range(GROUPS):
        ag[g // 3, 0, 0, g % 3] = buf[g, 0]
    ag_copy(0).start()
    ag_copy(1).start()
    kg_next(3)
    hidden_back(HALF, 0, 8)
    kg_next(4)
    mixed_back(pre, win1, HALF, 6, (2, 3))
    kg_next(5)
    ag_copy(0).wait_recv()
    ag_copy(1).wait_recv()
    ag_copy(2).start()
    ag_copy(3).start()
    mix_transposed(6, kt1, g2_row, put_out, (1, 2))
    kg_next(6)
    ag_copy(2).wait_recv()
    ag_copy(3).wait_recv()
    for n in (4, 5, 6, 7):
        ag_copy(n).start()
    halo_wait(4, mge.at[6], mge.at[11])
    mix_transposed(6, kt1, g2_row, put_out, (0, 3))
    for n in (4, 5, 6, 7):
        ag_copy(n).wait_recv()

    scale = 1.0 / 16.0
    for m, dst in ((0, ginv), (1, goutv)):
        mm = (m + yhi) % 2
        for q in range(4):
            qq = ((q // 2 + gx1) % 2) * 2 + (q % 2 + gx0) % 2
            for g in range(GROUPS):
                dst[q * SUB : (q + 1) * SUB, g * LANES : (g + 1) * LANES] = ag[g // 3, qq, mm, g % 3].astype(F32) * scale
    gkv[...] = kg[7, :9] * scale
    for n in range(6):
        halos[n].wait_send()
    for i in range(6):
        for g in range(GROUPS):
            rs_copy(i, g).wait_send()
    for n in range(8):
        ag_copy(n).wait_send()
    for t in range(7):
        kg_copy(t).wait_send()


def in_rows(a):
    return jnp.pad(a[0], ((0, 0), (0, PAD - LON), (0, 0)))


def in_order(a):
    rows = in_rows(a)
    return jnp.concatenate([rows[i] for i in ORDER], axis=0)


def step(mixed_two, input_two, cotangent, w_in_two, w_out_two, kernel_two, mixed_one, w_in_one, w_out_one, kernel_one):
    dma = pltpu.SemaphoreType.DMA
    here, far = pl.BlockSpec(memory_space=pltpu.VMEM), pl.BlockSpec(memory_space=pl.ANY)
    vmem = pltpu.VMEM
    tokens = (TOK, D)
    out, gin, gout, gk = pl.pallas_call(
        body,
        out_shape=(
            jax.ShapeDtypeStruct((1, 4, LON, D), BF16),
            jax.ShapeDtypeStruct((PAD, D), F32),
            jax.ShapeDtypeStruct((PAD, D), F32),
            jax.ShapeDtypeStruct((TAPS, D), F32),
        ),
        in_specs=[here, here, here, far, far, here, here, far, far, here],
        out_specs=[here] * 4,
        scratch_shapes=[
            vmem((2, PAD, D), BF16),
            vmem((FF, D), BF16), vmem((FF, D), BF16), vmem((FF, D), BF16),
            vmem((TOK, FF), BF16),
            vmem((12, PAD, D), BF16), vmem(tokens, BF16),
            vmem((8, 16, D), F32), vmem((7, 16, D), F32),
            vmem((2, 2, 8, GROUPS, SUB, LANES), BF16),
            vmem((SLOTS, 8, GROUPS, SUB, LANES), BF16),
            vmem((GROUPS, 64, SUB, LANES), BF16),
            vmem((GROUPS, 64, SUB, LANES), BF16),
            vmem((2, 4, 2, 3, SUB, LANES), BF16),
            dma((18,)), dma((STEPS,)), dma((STEPS,)), dma((6, GROUPS)), dma((6, GROUPS)),
            dma((8,)), dma((8,)), dma((7,)), dma((7,)), dma((6,)), dma((6,)),
        ],
        compiler_params=pltpu.CompilerParams(
            collective_id=0, has_side_effects=True, vmem_limit_bytes=VMEM_LIMIT
        ),
    )(
        in_order(mixed_two), in_rows(input_two), in_order(cotangent), w_in_two, w_out_two, kernel_two,
        in_order(mixed_one), w_in_one, w_out_one, kernel_one,
    )
    return out, gin, gout, gk


def solution(mesh):
    finer = Mesh(mesh.devices.reshape(2, 4, 2, 4, 2), AXES)
    grid = P(DP, SPACE, None, None)
    return jax.shard_map(
        step,
        mesh=finer,
        in_specs=(grid, grid, grid, P(), P(), P(), grid, P(), P(), P()),
        out_specs=(grid, P(DP, None), P(DP, None), P()),
        check_vma=False,
    )
```

```python
import math

import jax
import jax.numpy as jnp
from jax import lax
from jax.experimental import pallas as pl
from jax.experimental.pallas import tpu as pltpu
from jax.sharding import Mesh
from jax.sharding import PartitionSpec as P

AXES = ("space_0", "space_1", "dp_0", "dp_1", "dp_2")
SPACE = ("space_0", "space_1")
DP = ("dp_0", "dp_1", "dp_2")
MESH = pl.DeviceIdType.MESH
GELU_C = math.sqrt(2.0 / math.pi)
GELU_A = GELU_C * 0.044715
LAST = (((1,), (1,)), ((), ()))
F32 = jnp.float32
BF16 = jnp.bfloat16

D = 768
FF = 3072
LON = 180
PAD = 192
TOK = 4 * PAD
HALF = 2 * PAD
BLK = 384
STEPS = FF // BLK
SUB = 48
TAPS = 9
GROUPS = 6
LANES = 128
VMEM_LIMIT = 44 << 20
SLOTS = 4
ORDER = (0, 3, 1, 2)
PERM = (
    (5, 3, 1, 2, 0, 4),
    (3, 5, 0, 1, 2, 4),
    (1, 4, 3, 0, 2, 5),
    (4, 1, 2, 3, 0, 5),
    (2, 0, 5, 1, 3, 4),
    (0, 2, 4, 3, 1, 5),
)


def place_of(group, bits):
    where = 0
    for i, bit in enumerate(PERM[group]):
        where = where + bits[bit] * (1 << (5 - i))
    return where


def last_bits(group, n):
    return tuple(sorted(PERM[group][3 + i] for i in range(3) if n & (4 >> i)))


def gelu_all(v):
    v2 = v * v
    t = jnp.tanh(v * (GELU_C + GELU_A * v2))
    q = 0.5 + 0.5 * t
    slope = q + (v * (1.0 - t * t)) * (0.5 * GELU_C + (1.5 * GELU_A) * v2)
    return v * q, slope


def body(
    mx2, in2, ct, win2_h, wout2_h, k2_h, mx1, win1_h, wout1_h, k1_h,
    outv, ginv, goutv, gkv,
    inh, win2, wout2, win1, kt2, kt1,
    pre, mge, g2, kg, kgr,
    stage, d2d, buf, rcv, ag,
    load_sem, d2d_s, d2d_r, rs_s, rs_r, last_s, last_r, ag_s, ag_r, kg_s, kg_r, halo_s, halo_r,
):
    yhi = lax.axis_index("space_0")
    x = lax.axis_index("space_1")
    ylo = lax.axis_index("dp_0")
    z = lax.axis_index("dp_1")
    core = lax.axis_index("dp_2")
    gx1, gx0 = x // 2, (x // 2 + x) % 2
    gz1, gz0 = z // 2, (z // 2 + z) % 2
    def flipped(bits):
        xx, yy_hi, yy_lo, zz = x, yhi, ylo, z
        if 4 in bits:
            xx = 3 - xx
        if 5 in bits:
            xx = 2 * (xx // 2) + 1 - xx % 2
        if 0 in bits:
            zz = 3 - zz
        if 1 in bits:
            zz = 2 * (zz // 2) + 1 - zz % 2
        if 2 in bits:
            yy_hi, yy_lo = 1 - yy_hi, 1 - yy_lo
        if 3 in bits:
            yy_lo = 1 - yy_lo
        return (yy_hi, xx, yy_lo, zz, core)

    near = {
        "c": (yhi, x, ylo, z, 1 - core),
        "yy": (1 - yhi, x, ylo, z, core),
        "up": ((yhi + x // 3) % 2, (x + 1) % 4, ylo, z, core),
        "down": ((yhi + (3 - x) // 3) % 2, (x + 3) % 4, ylo, z, core),
    }
    for bit in range(6):
        near[bit] = flipped((bit,))
    for g in range(GROUPS):
        for n in range(1, 8):
            key = last_bits(g, n)
            if len(key) > 1 and key not in near:
                near[key] = flipped(key)
    first_band = (yhi * 4 + x) == 0
    last_band = (yhi * 4 + x) == 7

    def block_of(s):
        r = 7 - s
        a1, a0, c = r // 4, (r // 2) % 2, r % 2
        z1, z0 = (gz1 + a1) % 2, (gz0 + a0) % 2
        zz = 2 * z1 + (z1 + z0) % 2
        yy = (ylo + c) % 2
        rows = pl.multiple_of((yy * 4 + zz) * BLK, BLK)
        return rows, a1, a0, c

    other = pltpu.make_async_copy(win1_h, win1, load_sem.at[16])
    late = pltpu.make_async_copy(wout1_h, wout2, load_sem.at[17])

    def weight_copy(s, which):
        rows = pl.ds(block_of(s)[0], BLK)
        src, dst = ((win2_h, win2), (wout2_h, wout2))[which]
        return pltpu.make_async_copy(src.at[rows], dst.at[rows], load_sem.at[8 * which + s])

    for s in range(2):
        weight_copy(s, 0).start()
        weight_copy(s, 1).start()

    small = [
        pltpu.make_async_copy(k2_h, kt2, load_sem.at[18]),
        pltpu.make_async_copy(k1_h, kt1, load_sem.at[19]),
    ]

    barrier = pltpu.get_barrier_semaphore()
    for who in near.values():
        pl.semaphore_signal(barrier, inc=1, device_id=who, device_id_type=MESH)

    def remote(src, dst, ssem, rsem, who):
        return pltpu.make_async_remote_copy(
            src_ref=src, dst_ref=dst, send_sem=ssem, recv_sem=rsem, device_id=near[who], device_id_type=MESH
        )

    def core_copy(s):
        return remote(stage.at[s % 2, 1], d2d.at[s % SLOTS], d2d_s.at[s], d2d_r.at[s], "c")

    def core_add(s):
        rows, a1, a0, c = block_of(s)
        copy = core_copy(s)
        copy.wait_recv()
        for mq in range(8):
            m, q1, q0 = mq // 4, (mq // 2) % 2, mq % 2
            for g in range(GROUPS):
                at = place_of(g, (a1, a0, m, (c + m) % 2, q1, q0))
                buf[g, at] = stage[s % 2, 0, mq, g] + d2d[s % SLOTS, mq, g]
        copy.wait_send()
        first_sends(a1, a0, c)

    def pair_copy(g, a1, a0, c, m, u):
        x1, x0 = (0, u) if PERM[g][5] == 4 else (u, 0)
        at = pl.ds(place_of(g, (a1, a0, m, (c + m) % 2, x1, x0)), 2)
        return remote(buf.at[g, at], rcv.at[g, at], rs_s.at[0, g], rs_r.at[0, g], PERM[g][0])

    def first_sends(a1, a0, c):
        for g in range(GROUPS):
            bit = PERM[g][0]
            if bit in (4, 5):
                for m in range(2):
                    pair_copy(g, a1, a0, c, m, 1).start()
            elif bit in (2, 3):
                for u in range(2):
                    pair_copy(g, a1, a0, c, 1 if bit == 2 else 1 - c, u).start()

        for bit, flag in ((1, a0), (0, a1)):
            g = [p[0] for p in PERM].index(bit)
            if flag == 1:
                for m in range(2):
                    for u in range(2):
                        pair_copy(g, a1, a0, c, m, u).start()

    def rs_copy(i, g):
        half = pl.ds(1 << (5 - i), 1 << (5 - i))
        return remote(buf.at[g, half], rcv.at[g, half], rs_s.at[i, g], rs_r.at[i, g], PERM[g][i])

    def rs_send(i):
        for g in range(GROUPS):
            rs_copy(i, g).start()

    def rs_add(i):
        count = 1 << (5 - i)
        for g in range(GROUPS):
            rs_copy(i, g).wait_recv()

        @pl.loop(0, count)
        def _(n):
            for g in range(GROUPS):
                buf[g, n] = buf[g, n] + rcv[g, count + n]

    def last_copy(g, n):
        key = last_bits(g, n)
        who = key if len(key) > 1 else key[0]
        return remote(buf.at[g, n], rcv.at[g, n], last_s.at[g, n], last_r.at[g, n], who)

    def last_send():
        for n in range(1, 8):
            for g in range(GROUPS):
                last_copy(g, n).start()

    def last_add():
        for g in range(GROUPS):
            total = buf[g, 0].astype(F32)
            for n in range(1, 8):
                last_copy(g, n).wait_recv()
                total = total + rcv[g, n].astype(F32)
            ag[g // 3, 0, 0, g % 3] = total.astype(BF16)

    ag_list = [
        (0, (0, 0, 0), (0, 0, 1), "yy"),
        (1, (1, 0, 0), (1, 0, 1), "yy"),
        (2, (0, 0), (0, 1), 5),
        (3, (1, 0), (1, 2), 4),
        (4, (0, 0), (0, 2), 4),
        (5, (0, 1), (0, 3), 4),
        (6, (1, 0), (1, 1), 5),
        (7, (1, 2), (1, 3), 5),
    ]

    def ag_copy(n):
        _, src, dst, who = ag_list[n]
        return remote(ag.at[src], ag.at[dst], ag_s.at[n], ag_r.at[n], who)

    kg_bits = ("c", 5, 3, 1, 4, 2, 0)

    def kg_copy(t):
        return remote(kg.at[t], kgr.at[t], kg_s.at[t], kg_r.at[t], kg_bits[t])

    def kg_next(t):
        kg_copy(t).wait_recv()
        kg[t + 1] = kg[t] + kgr[t]
        if t + 1 < len(kg_bits):
            kg_copy(t + 1).start()

    halos = [
        remote(in2.at[0], inh.at[1], halo_s.at[0], halo_r.at[0], "down"),
        remote(in2.at[3], inh.at[0], halo_s.at[1], halo_r.at[1], "up"),
    ]
    for part in range(2):
        cols = pl.ds(part * (D // 2), D // 2)
        halos.append(remote(mge.at[1, :, cols], mge.at[5, :, cols], halo_s.at[2 * part + 2], halo_r.at[2 * part + 2], "down"))
        halos.append(remote(mge.at[4, :, cols], mge.at[0, :, cols], halo_s.at[2 * part + 3], halo_r.at[2 * part + 3], "up"))
    halos.append(remote(mge.at[7], mge.at[11], halo_s.at[6], halo_r.at[6], "down"))
    halos.append(remote(mge.at[10], mge.at[6], halo_s.at[7], halo_r.at[7], "up"))

    for s in range(STEPS):
        rows = pl.ds(block_of(s)[0], BLK)
        weight_copy(s, 0).wait()
        weight_copy(s, 1).wait()
        if s + 2 < STEPS:
            weight_copy(s + 2, 0).start()
            weight_copy(s + 2, 1).start()
        else:
            small[s + 2 - STEPS].start()
        if s == STEPS - 2:
            other.start()
        p = lax.dot_general(win2[rows, :], mx2[...], LAST, preferred_element_type=F32)
        h = lax.dot_general(wout2[rows, :], ct[...], LAST, preferred_element_type=F32)
        act, slope = gelu_all(p)
        pg = (h * slope).astype(BF16)
        terms = (
            jnp.dot(pg, mx2[...], preferred_element_type=F32).astype(BF16),
            jnp.dot(act.astype(BF16), ct[...], preferred_element_type=F32).astype(BF16),
        )
        pre[:, rows] = pg.T
        for m in range(2):
            mm = (m + yhi) % 2
            for half in range(2):
                slot = (half + core) % 2
                for q in range(4):
                    qq = ((q // 2 + gx1) % 2) * 2 + (q % 2 + gx0) % 2
                    lo = half * PAD + q * SUB
                    for g in range(GROUPS):
                        stage[s % 2, slot, mm * 4 + qq, g] = terms[m][lo : lo + SUB, g * LANES : (g + 1) * LANES]
        if s == 0:
            pl.semaphore_wait(barrier, len(near))
        core_copy(s).start()
        if s == 0:
            halos[0].start()
            halos[1].start()
        else:
            core_add(s - 1)

    late.start()

    def mixed_back(src, w, top, base, pair):
        @pl.loop(0, 3)
        def _(nb):
            cols = pl.ds(pl.multiple_of(nb * 256, 256), 256)
            r = jnp.dot(src[top : top + HALF, :], w[:, cols], preferred_element_type=F32).astype(BF16)
            mge[base + pair[0], :, cols] = r[:PAD]
            mge[base + pair[1], :, cols] = r[PAD:]

    def halo_wait(first, last, low, high):
        for n in range(first, last):
            halos[n].wait_recv()

        @pl.when(first_band)
        def _():
            low[...] = jnp.zeros((PAD, D), BF16)

        @pl.when(last_band)
        def _():
            high[...] = jnp.zeros((PAD, D), BF16)

    at_row = lax.broadcasted_iota(jnp.int32, (PAD, LANES), 0)

    def back(v):
        return jnp.where(at_row == LON - 1, v[0:1], pltpu.roll(v, PAD - 1, 0))

    def ahead(v):
        return jnp.where(at_row == 0, v[LON - 1 : LON], pltpu.roll(v, 1, 0))

    def kernel_gradient():
        kg[0, 8:16] = jnp.zeros((8, D), F32)

        @pl.loop(0, 6)
        def _(lb):
            cols = pl.ds(pl.multiple_of(lb * LANES, LANES), LANES)
            totals = [jnp.zeros((1, LANES), F32) for _ in range(9)]
            for i in range(4):
                v = jnp.where(at_row < LON, mge[i + 1, :, cols].astype(F32), 0.0)
                rolled = (back(v).astype(BF16), v.astype(BF16), ahead(v).astype(BF16))
                for a in range(3):
                    e = i + a - 1
                    field = inh[0, :, cols] if e < 0 else inh[1, :, cols] if e > 3 else in2[e, :, cols]
                    for b in range(3):
                        term = (field * rolled[b]).reshape(PAD // 16, 16, LANES)
                        part = term[0]
                        for n in range(1, PAD // 16):
                            part = part + term[n]
                        totals[3 * a + b] += part.astype(F32).sum(0, keepdims=True)
            for n in range(9):
                kg[0, n : n + 1, cols] = totals[n]

    def mix_transposed(base, kt, get, put, rows):
        @pl.loop(0, 6)
        def _(lb):
            cols = pl.ds(pl.multiple_of(lb * LANES, LANES), LANES)
            taps = kt[:, cols]
            for i in rows:
                sums = [None] * 3
                for a in range(3):
                    v = mge[base + i - a + 2, :, cols]
                    for b in range(3):
                        term = taps[3 * a + b : 3 * a + b + 1] * v
                        sums[b] = term if a == 0 else sums[b] + term
                sums = [t.astype(F32) for t in sums]
                put(i, cols, get(i, cols) + sums[1] + back(sums[0]) + ahead(sums[2]))

    def ct_row(i, cols):
        at = ORDER.index(i) * PAD
        return ct[at : at + PAD, cols].astype(F32)

    def g2_row(i, cols):
        at = ORDER.index(i) * PAD
        return g2[at : at + PAD, cols].astype(F32)

    def put_g2(i, cols, v):
        at = ORDER.index(i) * PAD
        g2[at : at + PAD, cols] = jnp.where(at_row < LON, v, 0.0).astype(BF16)

    def put_out(i, cols, v):
        outv[0, i, :, cols] = v[:LON].astype(BF16)

    def slopes_one(first, count):
        @pl.loop(first, first + count)
        def _(s):
            rows = pl.ds(pl.multiple_of(s * BLK, BLK), BLK)
            p = lax.dot_general(mx1[...], win1[rows, :], LAST, preferred_element_type=F32)
            pre[:, rows] = gelu_all(p)[1].astype(BF16)

    def hidden_back(top, first, count):
        @pl.loop(first, first + count)
        def _(s):
            rows = pl.ds(pl.multiple_of(s * BLK, BLK), BLK)
            h = lax.dot_general(g2[top : top + HALF, :], wout2[rows, :], LAST, preferred_element_type=F32)
            pre[top : top + HALF, rows] = (h * pre[top : top + HALF, rows].astype(F32)).astype(BF16)

    core_add(STEPS - 1)
    mixed_back(pre, win2, 0, 0, (1, 4))
    rs_add(0)
    rs_send(1)
    halos[2].start()
    halos[3].start()
    mixed_back(pre, win2, HALF, 0, (2, 3))
    other.wait()
    for copy in small:
        copy.wait()
    slopes_one(0, 4)
    mix_transposed(0, kt2, ct_row, put_g2, (1, 2))
    rs_add(1)
    rs_send(2)
    halos[4].start()
    halos[5].start()
    slopes_one(4, 4)
    halo_wait(0, 2, inh.at[0], inh.at[1])
    kernel_gradient()
    kg_copy(0).start()
    rs_add(2)
    last_send()
    halo_wait(2, 6, mge.at[0], mge.at[5])
    mix_transposed(0, kt2, ct_row, put_g2, (0, 3))
    late.wait()
    kg_next(0)
    hidden_back(0, 0, 8)
    kg_next(1)
    last_add()
    ag_copy(0).start()
    ag_copy(1).start()
    mixed_back(pre, win1, 0, 6, (1, 4))
    halos[6].start()
    halos[7].start()
    kg_next(2)
    hidden_back(HALF, 0, 8)
    kg_next(3)
    ag_copy(0).wait_recv()
    ag_copy(1).wait_recv()
    ag_copy(2).start()
    ag_copy(3).start()
    mixed_back(pre, win1, HALF, 6, (2, 3))
    kg_next(4)
    mix_transposed(6, kt1, g2_row, put_out, (1, 2))
    kg_next(5)
    ag_copy(2).wait_recv()
    ag_copy(3).wait_recv()
    for n in (4, 5, 6, 7):
        ag_copy(n).start()
    halo_wait(6, 8, mge.at[6], mge.at[11])
    mix_transposed(6, kt1, g2_row, put_out, (0, 3))
    kg_next(6)
    for n in (4, 5, 6, 7):
        ag_copy(n).wait_recv()

    for m, dst in ((0, ginv), (1, goutv)):
        mm = (m + yhi) % 2
        for q in range(4):
            qq = ((q // 2 + gx1) % 2) * 2 + (q % 2 + gx0) % 2
            for g in range(GROUPS):
                dst[q * SUB : (q + 1) * SUB, g * LANES : (g + 1) * LANES] = ag[g // 3, qq, mm, g % 3]
    gkv[...] = kg[7, :TAPS]
    for n in range(8):
        halos[n].wait_send()
    for i in range(3):
        for g in range(GROUPS):
            rs_copy(i, g).wait_send()
    for g in range(GROUPS):
        for n in range(1, 8):
            last_copy(g, n).wait_send()
    for n in range(8):
        ag_copy(n).wait_send()
    for t in range(7):
        kg_copy(t).wait_send()


def in_rows(a):
    return jnp.pad(a[0], ((0, 0), (0, PAD - LON), (0, 0)))


def in_order(a):
    rows = in_rows(a)
    return jnp.concatenate([rows[i] for i in ORDER], axis=0)


def step(mixed_two, input_two, cotangent, w_in_two, w_out_two, kernel_two, mixed_one, w_in_one, w_out_one, kernel_one):
    dma = pltpu.SemaphoreType.DMA
    here, far = pl.BlockSpec(memory_space=pltpu.VMEM), pl.BlockSpec(memory_space=pl.ANY)
    vmem = pltpu.VMEM
    tokens = (TOK, D)
    out, gin, gout, gk = pl.pallas_call(
        body,
        out_shape=(
            jax.ShapeDtypeStruct((1, 4, LON, D), BF16),
            jax.ShapeDtypeStruct((PAD, D), BF16),
            jax.ShapeDtypeStruct((PAD, D), BF16),
            jax.ShapeDtypeStruct((TAPS, D), F32),
        ),
        in_specs=[here, here, here, far, far, far, here, far, far, far],
        out_specs=[here] * 4,
        scratch_shapes=[
            vmem((2, PAD, D), BF16),
            vmem((FF, D), BF16), vmem((FF, D), BF16), vmem((FF, D), BF16),
            vmem((TAPS, D), BF16), vmem((TAPS, D), BF16),
            vmem((TOK, FF), BF16),
            vmem((12, PAD, D), BF16), vmem(tokens, BF16),
            vmem((8, 16, D), F32), vmem((7, 16, D), F32),
            vmem((2, 2, 8, GROUPS, SUB, LANES), BF16),
            vmem((SLOTS, 8, GROUPS, SUB, LANES), BF16),
            vmem((GROUPS, 64, SUB, LANES), BF16),
            vmem((GROUPS, 64, SUB, LANES), BF16),
            vmem((2, 4, 2, 3, SUB, LANES), BF16),
            dma((20,)), dma((STEPS,)), dma((STEPS,)), dma((3, GROUPS)), dma((3, GROUPS)), dma((GROUPS, 8)), dma((GROUPS, 8)),
            dma((8,)), dma((8,)), dma((7,)), dma((7,)), dma((8,)), dma((8,)),
        ],
        compiler_params=pltpu.CompilerParams(
            collective_id=0, has_side_effects=True, vmem_limit_bytes=VMEM_LIMIT
        ),
    )(
        in_order(mixed_two), in_rows(input_two), in_order(cotangent), w_in_two, w_out_two, kernel_two,
        in_order(mixed_one), w_in_one, w_out_one, kernel_one,
    )
    scale = 1.0 / 16.0
    return out, gin.astype(F32) * scale, gout.astype(F32) * scale, gk * scale


def solution(mesh):
    finer = Mesh(mesh.devices.reshape(2, 4, 2, 4, 2), AXES)
    grid = P(DP, SPACE, None, None)
    return jax.shard_map(
        step,
        mesh=finer,
        in_specs=(grid, grid, grid, P(), P(), P(), grid, P(), P(), P()),
        out_specs=(grid, P(DP, None), P(DP, None), P()),
        check_vma=False,
    )
```

```python
import math

import jax
import jax.numpy as jnp
from jax import lax
from jax.experimental import pallas as pl
from jax.experimental.pallas import tpu as pltpu
from jax.sharding import Mesh
from jax.sharding import PartitionSpec as P

AXES = ("space_0", "space_1", "dp_0", "dp_1", "dp_2")
SPACE = ("space_0", "space_1")
DP = ("dp_0", "dp_1", "dp_2")
MESH = pl.DeviceIdType.MESH
GELU_C = math.sqrt(2.0 / math.pi)
GELU_A = GELU_C * 0.044715
LAST = (((1,), (1,)), ((), ()))
F32 = jnp.float32
BF16 = jnp.bfloat16

D = 768
FF = 3072
LON = 180
PAD = 192
TOK = 4 * PAD
HALF = 2 * PAD
BLK = 384
STEPS = FF // BLK
SUB = 48
TAPS = 9
GROUPS = 6
LANES = 128
VMEM_LIMIT = 44 << 20
SLOTS = 4
ORDER = (0, 3, 1, 2)
PERM = (
    (5, 3, 1, 2, 0, 4),
    (3, 5, 0, 1, 2, 4),
    (1, 4, 3, 0, 2, 5),
    (4, 1, 2, 3, 0, 5),
    (2, 0, 5, 1, 3, 4),
    (0, 2, 4, 3, 1, 5),
)


def place_of(group, bits):
    where = 0
    for i, bit in enumerate(PERM[group]):
        where = where + bits[bit] * (1 << (5 - i))
    return where


def last_bits(group, n):
    return tuple(sorted(PERM[group][3 + i] for i in range(3) if n & (4 >> i)))


def gelu_all(v):
    v2 = v * v
    t = jnp.tanh(v * (GELU_C + GELU_A * v2))
    q = 0.5 + 0.5 * t
    slope = q + (v * (1.0 - t * t)) * (0.5 * GELU_C + (1.5 * GELU_A) * v2)
    return v * q, slope


def body(
    mx2, in2, ct, win2_h, wout2_h, k2_h, mx1, win1_h, wout1_h, k1_h,
    outv, ginv, goutv, gkv,
    inh, win2, wout2, win1, kt2, kt1,
    pre, mge, g2, kg, kgr,
    stage, d2d, buf, rcv, ag,
    load_sem, d2d_s, d2d_r, rs_s, rs_r, last_s, last_r, ag_s, ag_r, kg_s, kg_r, halo_s, halo_r,
):
    yhi = lax.axis_index("space_0")
    x = lax.axis_index("space_1")
    ylo = lax.axis_index("dp_0")
    z = lax.axis_index("dp_1")
    core = lax.axis_index("dp_2")
    gx1, gx0 = x // 2, (x // 2 + x) % 2
    gz1, gz0 = z // 2, (z // 2 + z) % 2
    def flipped(bits):
        xx, yy_hi, yy_lo, zz = x, yhi, ylo, z
        if 4 in bits:
            xx = 3 - xx
        if 5 in bits:
            xx = 2 * (xx // 2) + 1 - xx % 2
        if 0 in bits:
            zz = 3 - zz
        if 1 in bits:
            zz = 2 * (zz // 2) + 1 - zz % 2
        if 2 in bits:
            yy_hi, yy_lo = 1 - yy_hi, 1 - yy_lo
        if 3 in bits:
            yy_lo = 1 - yy_lo
        return (yy_hi, xx, yy_lo, zz, core)

    near = {
        "c": (yhi, x, ylo, z, 1 - core),
        "yy": (1 - yhi, x, ylo, z, core),
        "up": ((yhi + x // 3) % 2, (x + 1) % 4, ylo, z, core),
        "down": ((yhi + (3 - x) // 3) % 2, (x + 3) % 4, ylo, z, core),
    }
    for bit in range(6):
        near[bit] = flipped((bit,))
    for g in range(GROUPS):
        for n in range(1, 8):
            key = last_bits(g, n)
            if len(key) > 1 and key not in near:
                near[key] = flipped(key)
    first_band = (yhi * 4 + x) == 0
    last_band = (yhi * 4 + x) == 7

    def block_of(s):
        r = 7 - s
        a1, a0, c = r // 4, (r // 2) % 2, r % 2
        z1, z0 = (gz1 + a1) % 2, (gz0 + a0) % 2
        zz = 2 * z1 + (z1 + z0) % 2
        yy = (ylo + c) % 2
        rows = pl.multiple_of((yy * 4 + zz) * BLK, BLK)
        return rows, a1, a0, c

    other = pltpu.make_async_copy(win1_h, win1, load_sem.at[16])
    late = pltpu.make_async_copy(wout1_h, wout2, load_sem.at[17])

    def weight_copy(s, which):
        rows = pl.ds(block_of(s)[0], BLK)
        src, dst = ((win2_h, win2), (wout2_h, wout2))[which]
        return pltpu.make_async_copy(src.at[rows], dst.at[rows], load_sem.at[8 * which + s])

    for s in range(2):
        weight_copy(s, 0).start()
        weight_copy(s, 1).start()

    small = [
        pltpu.make_async_copy(k2_h, kt2, load_sem.at[18]),
        pltpu.make_async_copy(k1_h, kt1, load_sem.at[19]),
    ]

    barrier = pltpu.get_barrier_semaphore()
    for who in near.values():
        pl.semaphore_signal(barrier, inc=1, device_id=who, device_id_type=MESH)

    def remote(src, dst, ssem, rsem, who):
        return pltpu.make_async_remote_copy(
            src_ref=src, dst_ref=dst, send_sem=ssem, recv_sem=rsem, device_id=near[who], device_id_type=MESH
        )

    def core_copy(s):
        return remote(stage.at[s % 2, 1], d2d.at[s % SLOTS], d2d_s.at[s], d2d_r.at[s], "c")

    def core_add(s):
        rows, a1, a0, c = block_of(s)
        copy = core_copy(s)
        copy.wait_recv()
        for mq in range(8):
            m, q1, q0 = mq // 4, (mq // 2) % 2, mq % 2
            for g in range(GROUPS):
                at = place_of(g, (a1, a0, m, (c + m) % 2, q1, q0))
                buf[g, at] = stage[s % 2, 0, mq, g] + d2d[s % SLOTS, mq, g]
        copy.wait_send()
        first_sends(a1, a0, c)

    def pair_copy(g, a1, a0, c, m, u):
        x1, x0 = (0, u) if PERM[g][5] == 4 else (u, 0)
        at = pl.ds(place_of(g, (a1, a0, m, (c + m) % 2, x1, x0)), 2)
        return remote(buf.at[g, at], rcv.at[g, at], rs_s.at[0, g], rs_r.at[0, g], PERM[g][0])

    def first_sends(a1, a0, c):
        for g in range(GROUPS):
            bit = PERM[g][0]
            if bit in (4, 5):
                for m in range(2):
                    pair_copy(g, a1, a0, c, m, 1).start()
            elif bit in (2, 3):
                for u in range(2):
                    pair_copy(g, a1, a0, c, 1 if bit == 2 else 1 - c, u).start()

        for bit, flag in ((1, a0), (0, a1)):
            g = [p[0] for p in PERM].index(bit)
            if flag == 1:
                for m in range(2):
                    for u in range(2):
                        pair_copy(g, a1, a0, c, m, u).start()

    def rs_copy(i, g):
        half = pl.ds(1 << (5 - i), 1 << (5 - i))
        return remote(buf.at[g, half], rcv.at[g, half], rs_s.at[i, g], rs_r.at[i, g], PERM[g][i])

    def rs_send(i):
        for g in range(GROUPS):
            rs_copy(i, g).start()

    def rs_add(i):
        count = 1 << (5 - i)
        for g in range(GROUPS):
            rs_copy(i, g).wait_recv()

        @pl.loop(0, count)
        def _(n):
            for g in range(GROUPS):
                buf[g, n] = buf[g, n] + rcv[g, count + n]

    def last_copy(g, n):
        key = last_bits(g, n)
        who = key if len(key) > 1 else key[0]
        return remote(buf.at[g, n], rcv.at[g, n], last_s.at[g, n], last_r.at[g, n], who)

    def last_send():
        for n in range(1, 8):
            for g in range(GROUPS):
                last_copy(g, n).start()

    def last_add():
        for g in range(GROUPS):
            total = buf[g, 0].astype(F32)
            for n in range(1, 8):
                last_copy(g, n).wait_recv()
                total = total + rcv[g, n].astype(F32)
            ag[g // 3, 0, 0, g % 3] = total.astype(BF16)

    ag_list = [
        (0, (0, 0, 0), (0, 0, 1), "yy"),
        (1, (1, 0, 0), (1, 0, 1), "yy"),
        (2, (0, 0), (0, 1), 5),
        (3, (1, 0), (1, 2), 4),
        (4, (0, 0), (0, 2), 4),
        (5, (0, 1), (0, 3), 4),
        (6, (1, 0), (1, 1), 5),
        (7, (1, 2), (1, 3), 5),
    ]

    def ag_copy(n):
        _, src, dst, who = ag_list[n]
        return remote(ag.at[src], ag.at[dst], ag_s.at[n], ag_r.at[n], who)

    kg_bits = ("c", 5, 3, 1, 4, 2, 0)

    def kg_copy(t):
        return remote(kg.at[t], kgr.at[t], kg_s.at[t], kg_r.at[t], kg_bits[t])

    def kg_next(t):
        kg_copy(t).wait_recv()
        kg[t + 1] = kg[t] + kgr[t]
        if t + 1 < len(kg_bits):
            kg_copy(t + 1).start()

    halos = [
        remote(in2.at[0], inh.at[1], halo_s.at[0], halo_r.at[0], "down"),
        remote(in2.at[3], inh.at[0], halo_s.at[1], halo_r.at[1], "up"),
    ]
    for base in (0, 6):
        for part in range(2):
            cols = pl.ds(part * (D // 2), D // 2)
            n = len(halos)
            halos.append(remote(mge.at[base + 1, :, cols], mge.at[base + 5, :, cols], halo_s.at[n], halo_r.at[n], "down"))
            halos.append(remote(mge.at[base + 4, :, cols], mge.at[base, :, cols], halo_s.at[n + 1], halo_r.at[n + 1], "up"))

    for s in range(STEPS):
        rows = pl.ds(block_of(s)[0], BLK)
        weight_copy(s, 0).wait()
        weight_copy(s, 1).wait()
        if s + 2 < STEPS:
            weight_copy(s + 2, 0).start()
            weight_copy(s + 2, 1).start()
        else:
            small[s + 2 - STEPS].start()
        if s == STEPS - 2:
            other.start()
        p = lax.dot_general(win2[rows, :], mx2[...], LAST, preferred_element_type=F32)
        h = lax.dot_general(wout2[rows, :], ct[...], LAST, preferred_element_type=F32)
        act, slope = gelu_all(p)
        pg = (h * slope).astype(BF16)
        terms = (
            jnp.dot(pg, mx2[...], preferred_element_type=F32).astype(BF16),
            jnp.dot(act.astype(BF16), ct[...], preferred_element_type=F32).astype(BF16),
        )
        pre[:, rows] = pg.T
        for m in range(2):
            mm = (m + yhi) % 2
            for half in range(2):
                slot = (half + core) % 2
                for q in range(4):
                    qq = ((q // 2 + gx1) % 2) * 2 + (q % 2 + gx0) % 2
                    lo = half * PAD + q * SUB
                    for g in range(GROUPS):
                        stage[s % 2, slot, mm * 4 + qq, g] = terms[m][lo : lo + SUB, g * LANES : (g + 1) * LANES]
        if s == 0:
            pl.semaphore_wait(barrier, len(near))
        core_copy(s).start()
        if s == 0:
            halos[0].start()
            halos[1].start()
        else:
            core_add(s - 1)

    late.start()

    def mixed_back(src, w, top, base, pair):
        @pl.loop(0, 3)
        def _(nb):
            cols = pl.ds(pl.multiple_of(nb * 256, 256), 256)
            r = jnp.dot(src[top : top + HALF, :], w[:, cols], preferred_element_type=F32).astype(BF16)
            mge[base + pair[0], :, cols] = r[:PAD]
            mge[base + pair[1], :, cols] = r[PAD:]

    def halo_wait(first, last, low, high):
        for n in range(first, last):
            halos[n].wait_recv()

        @pl.when(first_band)
        def _():
            low[...] = jnp.zeros((PAD, D), BF16)

        @pl.when(last_band)
        def _():
            high[...] = jnp.zeros((PAD, D), BF16)

    at_row = lax.broadcasted_iota(jnp.int32, (PAD, LANES), 0)

    def back(v):
        return jnp.where(at_row == LON - 1, v[0:1], pltpu.roll(v, PAD - 1, 0))

    def ahead(v):
        return jnp.where(at_row == 0, v[LON - 1 : LON], pltpu.roll(v, 1, 0))

    def kernel_gradient():
        kg[0, 8:16] = jnp.zeros((8, D), F32)

        @pl.loop(0, 6)
        def _(lb):
            cols = pl.ds(pl.multiple_of(lb * LANES, LANES), LANES)
            totals = [jnp.zeros((1, LANES), F32) for _ in range(9)]
            for i in range(4):
                v = jnp.where(at_row < LON, mge[i + 1, :, cols].astype(F32), 0.0)
                rolled = (back(v).astype(BF16), v.astype(BF16), ahead(v).astype(BF16))
                for a in range(3):
                    e = i + a - 1
                    field = inh[0, :, cols] if e < 0 else inh[1, :, cols] if e > 3 else in2[e, :, cols]
                    for b in range(3):
                        term = (field * rolled[b]).reshape(PAD // 16, 16, LANES)
                        part = term[0]
                        for n in range(1, PAD // 16):
                            part = part + term[n]
                        totals[3 * a + b] += part.astype(F32).sum(0, keepdims=True)
            for n in range(9):
                kg[0, n : n + 1, cols] = totals[n]

    def mix_transposed(base, kt, get, put, rows):
        @pl.loop(0, 6)
        def _(lb):
            cols = pl.ds(pl.multiple_of(lb * LANES, LANES), LANES)
            taps = kt[:, cols]
            for i in rows:
                sums = [None] * 3
                for a in range(3):
                    v = mge[base + i - a + 2, :, cols]
                    for b in range(3):
                        term = taps[3 * a + b : 3 * a + b + 1] * v
                        sums[b] = term if a == 0 else sums[b] + term
                sums = [t.astype(F32) for t in sums]
                put(i, cols, get(i, cols) + sums[1] + back(sums[0]) + ahead(sums[2]))

    def ct_row(i, cols):
        at = ORDER.index(i) * PAD
        return ct[at : at + PAD, cols].astype(F32)

    def g2_row(i, cols):
        at = ORDER.index(i) * PAD
        return g2[at : at + PAD, cols].astype(F32)

    def put_g2(i, cols, v):
        at = ORDER.index(i) * PAD
        g2[at : at + PAD, cols] = jnp.where(at_row < LON, v, 0.0).astype(BF16)

    def put_out(i, cols, v):
        outv[0, i, :, cols] = v[:LON].astype(BF16)

    def slopes_one(first, count):
        @pl.loop(first, first + count)
        def _(s):
            rows = pl.ds(pl.multiple_of(s * BLK, BLK), BLK)
            p = lax.dot_general(mx1[...], win1[rows, :], LAST, preferred_element_type=F32)
            pre[:, rows] = gelu_all(p)[1].astype(BF16)

    def hidden_back(top, first, count):
        @pl.loop(first, first + count)
        def _(s):
            rows = pl.ds(pl.multiple_of(s * BLK, BLK), BLK)
            h = lax.dot_general(g2[top : top + HALF, :], wout2[rows, :], LAST, preferred_element_type=F32)
            pre[top : top + HALF, rows] = (h * pre[top : top + HALF, rows].astype(F32)).astype(BF16)

    core_add(STEPS - 1)
    mixed_back(pre, win2, 0, 0, (1, 4))
    rs_add(0)
    rs_send(1)
    halos[2].start()
    halos[3].start()
    mixed_back(pre, win2, HALF, 0, (2, 3))
    other.wait()
    for copy in small:
        copy.wait()
    slopes_one(0, 4)
    mix_transposed(0, kt2, ct_row, put_g2, (1, 2))
    rs_add(1)
    rs_send(2)
    halos[4].start()
    halos[5].start()
    slopes_one(4, 4)
    rs_add(2)
    last_send()
    halo_wait(0, 2, inh.at[0], inh.at[1])
    kernel_gradient()
    kg_copy(0).start()
    halo_wait(2, 6, mge.at[0], mge.at[5])
    mix_transposed(0, kt2, ct_row, put_g2, (0, 3))
    late.wait()
    kg_next(0)
    hidden_back(0, 0, 8)
    kg_next(1)
    last_add()
    ag_copy(0).start()
    ag_copy(1).start()
    mixed_back(pre, win1, 0, 6, (1, 4))
    halos[6].start()
    halos[7].start()
    kg_next(2)
    hidden_back(HALF, 0, 8)
    kg_next(3)
    ag_copy(0).wait_recv()
    ag_copy(1).wait_recv()
    ag_copy(2).start()
    ag_copy(3).start()
    halos[8].start()
    halos[9].start()
    mixed_back(pre, win1, HALF, 6, (2, 3))
    kg_next(4)
    mix_transposed(6, kt1, g2_row, put_out, (1, 2))
    kg_next(5)
    ag_copy(2).wait_recv()
    ag_copy(3).wait_recv()
    for n in (4, 5, 6, 7):
        ag_copy(n).start()
    halo_wait(6, 10, mge.at[6], mge.at[11])
    mix_transposed(6, kt1, g2_row, put_out, (0, 3))
    kg_next(6)
    for n in (4, 5, 6, 7):
        ag_copy(n).wait_recv()

    for m, dst in ((0, ginv), (1, goutv)):
        mm = (m + yhi) % 2
        for q in range(4):
            qq = ((q // 2 + gx1) % 2) * 2 + (q % 2 + gx0) % 2
            for g in range(GROUPS):
                dst[q * SUB : (q + 1) * SUB, g * LANES : (g + 1) * LANES] = ag[g // 3, qq, mm, g % 3]
    gkv[...] = kg[7, :TAPS]
    for n in range(10):
        halos[n].wait_send()
    for i in range(3):
        for g in range(GROUPS):
            rs_copy(i, g).wait_send()
    for g in range(GROUPS):
        for n in range(1, 8):
            last_copy(g, n).wait_send()
    for n in range(8):
        ag_copy(n).wait_send()
    for t in range(7):
        kg_copy(t).wait_send()


def fields_in(*fields):
    every = lax.optimization_barrier(jnp.concatenate([f.transpose(0, 2, 1, 3) for f in fields], axis=0))
    rows = jnp.pad(every.transpose(0, 2, 1, 3), ((0, 0), (0, 0), (0, PAD - LON), (0, 0)))
    ordered = [jnp.concatenate([rows[n, i] for i in ORDER], axis=0) for n in range(3)]
    return ordered[0], ordered[1], ordered[2], rows[3]


def step(mixed_two, input_two, cotangent, w_in_two, w_out_two, kernel_two, mixed_one, w_in_one, w_out_one, kernel_one):
    dma = pltpu.SemaphoreType.DMA
    here, far = pl.BlockSpec(memory_space=pltpu.VMEM), pl.BlockSpec(memory_space=pl.ANY)
    vmem = pltpu.VMEM
    tokens = (TOK, D)
    mx2, ct, mx1, in2 = fields_in(mixed_two, cotangent, mixed_one, input_two)
    out, gin, gout, gk = pl.pallas_call(
        body,
        out_shape=(
            jax.ShapeDtypeStruct((1, 4, LON, D), BF16),
            jax.ShapeDtypeStruct((PAD, D), BF16),
            jax.ShapeDtypeStruct((PAD, D), BF16),
            jax.ShapeDtypeStruct((TAPS, D), F32),
        ),
        in_specs=[here, here, here, far, far, far, here, far, far, far],
        out_specs=[here] * 4,
        scratch_shapes=[
            vmem((2, PAD, D), BF16),
            vmem((FF, D), BF16), vmem((FF, D), BF16), vmem((FF, D), BF16),
            vmem((TAPS, D), BF16), vmem((TAPS, D), BF16),
            vmem((TOK, FF), BF16),
            vmem((12, PAD, D), BF16), vmem(tokens, BF16),
            vmem((8, 16, D), F32), vmem((7, 16, D), F32),
            vmem((2, 2, 8, GROUPS, SUB, LANES), BF16),
            vmem((SLOTS, 8, GROUPS, SUB, LANES), BF16),
            vmem((GROUPS, 64, SUB, LANES), BF16),
            vmem((GROUPS, 64, SUB, LANES), BF16),
            vmem((2, 4, 2, 3, SUB, LANES), BF16),
            dma((20,)), dma((STEPS,)), dma((STEPS,)), dma((3, GROUPS)), dma((3, GROUPS)), dma((GROUPS, 8)), dma((GROUPS, 8)),
            dma((8,)), dma((8,)), dma((7,)), dma((7,)), dma((10,)), dma((10,)),
        ],
        compiler_params=pltpu.CompilerParams(
            collective_id=0, has_side_effects=True, vmem_limit_bytes=VMEM_LIMIT
        ),
    )(
        mx2, in2, ct, w_in_two, w_out_two, kernel_two, mx1, w_in_one, w_out_one, kernel_one,
    )
    scale = 1.0 / 16.0
    return out, gin.astype(F32) * scale, gout.astype(F32) * scale, gk * scale


def solution(mesh):
    finer = Mesh(mesh.devices.reshape(2, 4, 2, 4, 2), AXES)
    grid = P(DP, SPACE, None, None)
    return jax.shard_map(
        step,
        mesh=finer,
        in_specs=(grid, grid, grid, P(), P(), P(), grid, P(), P(), P()),
        out_specs=(grid, P(DP, None), P(DP, None), P()),
        check_vma=False,
    )
```

```python
import math

import jax
import jax.numpy as jnp
from jax import lax
from jax.experimental import pallas as pl
from jax.experimental.pallas import tpu as pltpu
from jax.sharding import Mesh
from jax.sharding import PartitionSpec as P

AXES = ("space_0", "space_1", "dp_0", "dp_1", "dp_2")
SPACE = ("space_0", "space_1")
DP = ("dp_0", "dp_1", "dp_2")
MESH = pl.DeviceIdType.MESH
GELU_C = math.sqrt(2.0 / math.pi)
GELU_A = GELU_C * 0.044715
LAST = (((1,), (1,)), ((), ()))
F32 = jnp.float32
BF16 = jnp.bfloat16

D = 768
FF = 3072
LON = 180
PAD = 192
TOK = 4 * PAD
HALF = 2 * PAD
BLK = 384
STEPS = FF // BLK
SUB = 48
TAPS = 9
GROUPS = 6
LANES = 128
VMEM_LIMIT = 44 << 20
SLOTS = 4
ORDER = (0, 3, 1, 2)
PERM = (
    (5, 3, 1, 2, 0, 4),
    (3, 5, 0, 1, 2, 4),
    (1, 4, 3, 0, 2, 5),
    (4, 1, 2, 3, 0, 5),
    (2, 0, 5, 1, 3, 4),
    (0, 2, 4, 3, 1, 5),
)


def place_of(group, bits):
    where = 0
    for i, bit in enumerate(PERM[group]):
        where = where + bits[bit] * (1 << (5 - i))
    return where


def last_bits(group, n):
    return tuple(sorted(PERM[group][3 + i] for i in range(3) if n & (4 >> i)))


def gelu_all(v):
    v2 = v * v
    t = jnp.tanh(v * (GELU_C + GELU_A * v2))
    q = 0.5 + 0.5 * t
    slope = q + (v * (1.0 - t * t)) * (0.5 * GELU_C + (1.5 * GELU_A) * v2)
    return v * q, slope


def body(
    mx2, in2, ct, win2_h, wout2_h, k2_h, mx1, win1_h, wout1_h, k1_h,
    outv, ginv, goutv, gkv,
    inh, win2, wout2, win1, kt2, kt1,
    pre, mge, g2, kg, kgr,
    stage, d2d, buf, rcv, ag,
    load_sem, d2d_s, d2d_r, rs_s, rs_r, last_s, last_r, ag_s, ag_r, kg_s, kg_r, halo_s, halo_r,
):
    yhi = lax.axis_index("space_0")
    x = lax.axis_index("space_1")
    ylo = lax.axis_index("dp_0")
    z = lax.axis_index("dp_1")
    core = lax.axis_index("dp_2")
    gx1, gx0 = x // 2, (x // 2 + x) % 2
    gz1, gz0 = z // 2, (z // 2 + z) % 2
    def flipped(bits):
        xx, yy_hi, yy_lo, zz = x, yhi, ylo, z
        if 4 in bits:
            xx = 3 - xx
        if 5 in bits:
            xx = 2 * (xx // 2) + 1 - xx % 2
        if 0 in bits:
            zz = 3 - zz
        if 1 in bits:
            zz = 2 * (zz // 2) + 1 - zz % 2
        if 2 in bits:
            yy_hi, yy_lo = 1 - yy_hi, 1 - yy_lo
        if 3 in bits:
            yy_lo = 1 - yy_lo
        return (yy_hi, xx, yy_lo, zz, core)

    near = {
        "c": (yhi, x, ylo, z, 1 - core),
        "yy": (1 - yhi, x, ylo, z, core),
        "up": ((yhi + x // 3) % 2, (x + 1) % 4, ylo, z, core),
        "down": ((yhi + (3 - x) // 3) % 2, (x + 3) % 4, ylo, z, core),
    }
    for bit in range(6):
        near[bit] = flipped((bit,))
    for g in range(GROUPS):
        for n in range(1, 8):
            key = last_bits(g, n)
            if len(key) > 1 and key not in near:
                near[key] = flipped(key)
    first_band = (yhi * 4 + x) == 0
    last_band = (yhi * 4 + x) == 7

    def block_of(s):
        r = 7 - s
        a1, a0, c = r // 4, (r // 2) % 2, r % 2
        z1, z0 = (gz1 + a1) % 2, (gz0 + a0) % 2
        zz = 2 * z1 + (z1 + z0) % 2
        yy = (ylo + c) % 2
        rows = pl.multiple_of((yy * 4 + zz) * BLK, BLK)
        return rows, a1, a0, c

    other = pltpu.make_async_copy(win1_h, win1, load_sem.at[16])
    late = pltpu.make_async_copy(wout1_h, wout2, load_sem.at[17])

    def weight_copy(s, which):
        rows = pl.ds(block_of(s)[0], BLK)
        src, dst = ((win2_h, win2), (wout2_h, wout2))[which]
        return pltpu.make_async_copy(src.at[rows], dst.at[rows], load_sem.at[8 * which + s])

    for s in range(2):
        weight_copy(s, 0).start()
        weight_copy(s, 1).start()

    small = [
        pltpu.make_async_copy(k2_h, kt2, load_sem.at[18]),
        pltpu.make_async_copy(k1_h, kt1, load_sem.at[19]),
    ]

    barrier = pltpu.get_barrier_semaphore()
    for who in near.values():
        pl.semaphore_signal(barrier, inc=1, device_id=who, device_id_type=MESH)

    def remote(src, dst, ssem, rsem, who):
        return pltpu.make_async_remote_copy(
            src_ref=src, dst_ref=dst, send_sem=ssem, recv_sem=rsem, device_id=near[who], device_id_type=MESH
        )

    def core_copy(s):
        return remote(stage.at[s % 2, 1], d2d.at[s % SLOTS], d2d_s.at[s], d2d_r.at[s], "c")

    def core_add(s):
        rows, a1, a0, c = block_of(s)
        copy = core_copy(s)
        copy.wait_recv()
        for mq in range(8):
            m, q1, q0 = mq // 4, (mq // 2) % 2, mq % 2
            for g in range(GROUPS):
                at = place_of(g, (a1, a0, m, (c + m) % 2, q1, q0))
                buf[g, at] = stage[s % 2, 0, mq, g] + d2d[s % SLOTS, mq, g]
        copy.wait_send()
        first_sends(a1, a0, c)

    def pair_copy(g, a1, a0, c, m, u):
        x1, x0 = (0, u) if PERM[g][5] == 4 else (u, 0)
        at = pl.ds(place_of(g, (a1, a0, m, (c + m) % 2, x1, x0)), 2)
        return remote(buf.at[g, at], rcv.at[g, at], rs_s.at[0, g], rs_r.at[0, g], PERM[g][0])

    def first_sends(a1, a0, c):
        for g in range(GROUPS):
            bit = PERM[g][0]
            if bit in (4, 5):
                for m in range(2):
                    pair_copy(g, a1, a0, c, m, 1).start()
            elif bit in (2, 3):
                for u in range(2):
                    pair_copy(g, a1, a0, c, 1 if bit == 2 else 1 - c, u).start()

        for bit, flag in ((1, a0), (0, a1)):
            g = [p[0] for p in PERM].index(bit)
            if flag == 1:
                for m in range(2):
                    for u in range(2):
                        pair_copy(g, a1, a0, c, m, u).start()

    def rs_copy(i, g):
        half = pl.ds(1 << (5 - i), 1 << (5 - i))
        return remote(buf.at[g, half], rcv.at[g, half], rs_s.at[i, g], rs_r.at[i, g], PERM[g][i])

    def last_copy(g, n):
        key = last_bits(g, n)
        who = key if len(key) > 1 else key[0]
        return remote(buf.at[g, n], rcv.at[g, n], last_s.at[g, n], last_r.at[g, n], who)

    def rs_step(i):
        count = 1 << (5 - i)
        for g in sorted(range(GROUPS), key=lambda n: PERM[n][i] in (4, 5)):
            rs_copy(i, g).wait_recv()

            @pl.loop(0, count // 4)
            def _(n):
                kept, come = pl.ds(n * 4, 4), pl.ds(count + n * 4, 4)
                buf[g, kept] = buf[g, kept] + rcv[g, come]

            if i < 2:
                rs_copy(i + 1, g).start()
            else:
                for n in range(1, 8):
                    last_copy(g, n).start()

    def last_add():
        for g in range(GROUPS):
            total = buf[g, 0].astype(F32)
            for n in range(1, 8):
                last_copy(g, n).wait_recv()
                total = total + rcv[g, n].astype(F32)
            ag[g // 3, 0, 0, g % 3] = total.astype(BF16)

    ag_list = [
        (0, (0, 0, 0), (0, 0, 1), "yy"),
        (1, (1, 0, 0), (1, 0, 1), "yy"),
        (2, (0, 0), (0, 1), 5),
        (3, (1, 0), (1, 2), 4),
        (4, (0, 0), (0, 2), 4),
        (5, (0, 1), (0, 3), 4),
        (6, (1, 0), (1, 1), 5),
        (7, (1, 2), (1, 3), 5),
    ]

    def ag_copy(n):
        _, src, dst, who = ag_list[n]
        return remote(ag.at[src], ag.at[dst], ag_s.at[n], ag_r.at[n], who)

    kg_bits = ("c", 5, 4, 3, 1, 2, 0)

    def kg_copy(t):
        return remote(kg.at[t], kgr.at[t], kg_s.at[t], kg_r.at[t], kg_bits[t])

    def kg_next(t):
        kg_copy(t).wait_recv()
        kg[t + 1] = kg[t] + kgr[t]
        if t + 1 < len(kg_bits):
            kg_copy(t + 1).start()

    halos = [
        remote(in2.at[0], inh.at[1], halo_s.at[0], halo_r.at[0], "down"),
        remote(in2.at[3], inh.at[0], halo_s.at[1], halo_r.at[1], "up"),
    ]
    for base in (0, 6):
        for part in range(2):
            cols = pl.ds(part * (D // 2), D // 2)
            n = len(halos)
            halos.append(remote(mge.at[base + 1, :, cols], mge.at[base + 5, :, cols], halo_s.at[n], halo_r.at[n], "down"))
            halos.append(remote(mge.at[base + 4, :, cols], mge.at[base, :, cols], halo_s.at[n + 1], halo_r.at[n + 1], "up"))

    for s in range(STEPS):
        rows = pl.ds(block_of(s)[0], BLK)
        weight_copy(s, 0).wait()
        weight_copy(s, 1).wait()
        if s + 2 < STEPS:
            weight_copy(s + 2, 0).start()
            weight_copy(s + 2, 1).start()
        else:
            small[s + 2 - STEPS].start()
        if s == STEPS - 2:
            other.start()
        p = lax.dot_general(win2[rows, :], mx2[...], LAST, preferred_element_type=F32)
        h = lax.dot_general(wout2[rows, :], ct[...], LAST, preferred_element_type=F32)
        act, slope = gelu_all(p)
        pg = (h * slope).astype(BF16)
        terms = (
            jnp.dot(pg, mx2[...], preferred_element_type=F32).astype(BF16),
            jnp.dot(act.astype(BF16), ct[...], preferred_element_type=F32).astype(BF16),
        )
        pre[:, rows] = pg.T
        for m in range(2):
            mm = (m + yhi) % 2
            for half in range(2):
                slot = (half + core) % 2
                for q in range(4):
                    qq = ((q // 2 + gx1) % 2) * 2 + (q % 2 + gx0) % 2
                    lo = half * PAD + q * SUB
                    for g in range(GROUPS):
                        stage[s % 2, slot, mm * 4 + qq, g] = terms[m][lo : lo + SUB, g * LANES : (g + 1) * LANES]
        if s == 0:
            pl.semaphore_wait(barrier, len(near))
        core_copy(s).start()
        if s == 0:
            halos[0].start()
            halos[1].start()
        else:
            core_add(s - 1)

    late.start()

    def mixed_back(src, w, top, base, pair):
        @pl.loop(0, 3)
        def _(nb):
            cols = pl.ds(pl.multiple_of(nb * 256, 256), 256)
            r = jnp.dot(src[top : top + HALF, :], w[:, cols], preferred_element_type=F32).astype(BF16)
            mge[base + pair[0], :, cols] = r[:PAD]
            mge[base + pair[1], :, cols] = r[PAD:]

    def halo_wait(first, last, low, high):
        for n in range(first, last):
            halos[n].wait_recv()

        @pl.when(first_band)
        def _():
            low[...] = jnp.zeros((PAD, D), BF16)

        @pl.when(last_band)
        def _():
            high[...] = jnp.zeros((PAD, D), BF16)

    at_row = lax.broadcasted_iota(jnp.int32, (PAD, LANES), 0)

    def back(v):
        return jnp.where(at_row == LON - 1, v[0:1], pltpu.roll(v, PAD - 1, 0))

    def ahead(v):
        return jnp.where(at_row == 0, v[LON - 1 : LON], pltpu.roll(v, 1, 0))

    def kernel_gradient():
        kg[0, 8:16] = jnp.zeros((8, D), F32)

        @pl.loop(0, 6)
        def _(lb):
            cols = pl.ds(pl.multiple_of(lb * LANES, LANES), LANES)
            totals = [jnp.zeros((1, LANES), F32) for _ in range(9)]
            for i in range(4):
                v = jnp.where(at_row < LON, mge[i + 1, :, cols].astype(F32), 0.0)
                rolled = (back(v).astype(BF16), v.astype(BF16), ahead(v).astype(BF16))
                for a in range(3):
                    e = i + a - 1
                    field = inh[0, :, cols] if e < 0 else inh[1, :, cols] if e > 3 else in2[e, :, cols]
                    for b in range(3):
                        term = (field * rolled[b]).reshape(PAD // 16, 16, LANES)
                        part = term[0]
                        for n in range(1, PAD // 16):
                            part = part + term[n]
                        totals[3 * a + b] += part.astype(F32).sum(0, keepdims=True)
            for n in range(9):
                kg[0, n : n + 1, cols] = totals[n]

    def mix_transposed(base, kt, get, put, rows):
        @pl.loop(0, 6)
        def _(lb):
            cols = pl.ds(pl.multiple_of(lb * LANES, LANES), LANES)
            taps = kt[:, cols]
            for i in rows:
                sums = [None] * 3
                for a in range(3):
                    v = mge[base + i - a + 2, :, cols]
                    for b in range(3):
                        term = taps[3 * a + b : 3 * a + b + 1] * v
                        sums[b] = term if a == 0 else sums[b] + term
                sums = [t.astype(F32) for t in sums]
                put(i, cols, get(i, cols) + sums[1] + back(sums[0]) + ahead(sums[2]))

    def ct_row(i, cols):
        at = ORDER.index(i) * PAD
        return ct[at : at + PAD, cols].astype(F32)

    def g2_row(i, cols):
        at = ORDER.index(i) * PAD
        return g2[at : at + PAD, cols].astype(F32)

    def put_g2(i, cols, v):
        at = ORDER.index(i) * PAD
        g2[at : at + PAD, cols] = jnp.where(at_row < LON, v, 0.0).astype(BF16)

    def put_out(i, cols, v):
        outv[0, i, :, cols] = v[:LON].astype(BF16)

    def slopes_one(first, count):
        @pl.loop(first, first + count)
        def _(s):
            rows = pl.ds(pl.multiple_of(s * BLK, BLK), BLK)
            p = lax.dot_general(mx1[...], win1[rows, :], LAST, preferred_element_type=F32)
            pre[:, rows] = gelu_all(p)[1].astype(BF16)

    def hidden_back(top, first, count):
        @pl.loop(first, first + count)
        def _(s):
            rows = pl.ds(pl.multiple_of(s * BLK, BLK), BLK)
            h = lax.dot_general(g2[top : top + HALF, :], wout2[rows, :], LAST, preferred_element_type=F32)
            pre[top : top + HALF, rows] = (h * pre[top : top + HALF, rows].astype(F32)).astype(BF16)

    core_add(STEPS - 1)
    mixed_back(pre, win2, 0, 0, (1, 4))
    rs_step(0)
    halos[2].start()
    halos[3].start()
    mixed_back(pre, win2, HALF, 0, (2, 3))
    other.wait()
    for copy in small:
        copy.wait()
    slopes_one(0, 4)
    mix_transposed(0, kt2, ct_row, put_g2, (1, 2))
    rs_step(1)
    halos[4].start()
    halos[5].start()
    slopes_one(4, 4)
    rs_step(2)
    halo_wait(0, 2, inh.at[0], inh.at[1])
    kernel_gradient()
    kg_copy(0).start()
    halo_wait(2, 6, mge.at[0], mge.at[5])
    mix_transposed(0, kt2, ct_row, put_g2, (0, 3))
    late.wait()
    kg_next(0)
    hidden_back(0, 0, 8)
    kg_next(1)
    last_add()
    ag_copy(0).start()
    ag_copy(1).start()
    mixed_back(pre, win1, 0, 6, (1, 4))
    halos[6].start()
    halos[7].start()
    kg_next(2)
    hidden_back(HALF, 0, 8)
    kg_next(3)
    ag_copy(0).wait_recv()
    ag_copy(1).wait_recv()
    ag_copy(2).start()
    ag_copy(3).start()
    halos[8].start()
    halos[9].start()
    mixed_back(pre, win1, HALF, 6, (2, 3))
    kg_next(4)
    mix_transposed(6, kt1, g2_row, put_out, (1, 2))
    kg_next(5)
    ag_copy(2).wait_recv()
    ag_copy(3).wait_recv()
    for n in (4, 5, 6, 7):
        ag_copy(n).start()
    halo_wait(6, 10, mge.at[6], mge.at[11])
    mix_transposed(6, kt1, g2_row, put_out, (0, 3))
    kg_next(6)
    for n in (4, 5, 6, 7):
        ag_copy(n).wait_recv()

    for m, dst in ((0, ginv), (1, goutv)):
        mm = (m + yhi) % 2
        for q in range(4):
            qq = ((q // 2 + gx1) % 2) * 2 + (q % 2 + gx0) % 2
            for g in range(GROUPS):
                dst[q * SUB : (q + 1) * SUB, g * LANES : (g + 1) * LANES] = ag[g // 3, qq, mm, g % 3]
    gkv[...] = kg[7, :TAPS]
    for n in range(10):
        halos[n].wait_send()
    for i in range(3):
        for g in range(GROUPS):
            rs_copy(i, g).wait_send()
    for g in range(GROUPS):
        for n in range(1, 8):
            last_copy(g, n).wait_send()
    for n in range(8):
        ag_copy(n).wait_send()
    for t in range(7):
        kg_copy(t).wait_send()


def fields_in(*fields):
    every = lax.optimization_barrier(jnp.concatenate([f.transpose(0, 2, 1, 3) for f in fields], axis=0))
    rows = jnp.pad(every.transpose(0, 2, 1, 3), ((0, 0), (0, 0), (0, PAD - LON), (0, 0)))
    ordered = [jnp.concatenate([rows[n, i] for i in ORDER], axis=0) for n in range(3)]
    return ordered[0], ordered[1], ordered[2], rows[3]


def step(mixed_two, input_two, cotangent, w_in_two, w_out_two, kernel_two, mixed_one, w_in_one, w_out_one, kernel_one):
    dma = pltpu.SemaphoreType.DMA
    here, far = pl.BlockSpec(memory_space=pltpu.VMEM), pl.BlockSpec(memory_space=pl.ANY)
    vmem = pltpu.VMEM
    tokens = (TOK, D)
    mx2, ct, mx1, in2 = fields_in(mixed_two, cotangent, mixed_one, input_two)
    out, gin, gout, gk = pl.pallas_call(
        body,
        out_shape=(
            jax.ShapeDtypeStruct((1, 4, LON, D), BF16),
            jax.ShapeDtypeStruct((PAD, D), BF16),
            jax.ShapeDtypeStruct((PAD, D), BF16),
            jax.ShapeDtypeStruct((TAPS, D), F32),
        ),
        in_specs=[here, here, here, far, far, far, here, far, far, far],
        out_specs=[here] * 4,
        scratch_shapes=[
            vmem((2, PAD, D), BF16),
            vmem((FF, D), BF16), vmem((FF, D), BF16), vmem((FF, D), BF16),
            vmem((TAPS, D), BF16), vmem((TAPS, D), BF16),
            vmem((TOK, FF), BF16),
            vmem((12, PAD, D), BF16), vmem(tokens, BF16),
            vmem((8, 16, D), F32), vmem((7, 16, D), F32),
            vmem((2, 2, 8, GROUPS, SUB, LANES), BF16),
            vmem((SLOTS, 8, GROUPS, SUB, LANES), BF16),
            vmem((GROUPS, 64, SUB, LANES), BF16),
            vmem((GROUPS, 64, SUB, LANES), BF16),
            vmem((2, 4, 2, 3, SUB, LANES), BF16),
            dma((20,)), dma((STEPS,)), dma((STEPS,)), dma((3, GROUPS)), dma((3, GROUPS)), dma((GROUPS, 8)), dma((GROUPS, 8)),
            dma((8,)), dma((8,)), dma((7,)), dma((7,)), dma((10,)), dma((10,)),
        ],
        compiler_params=pltpu.CompilerParams(
            collective_id=0, has_side_effects=True, vmem_limit_bytes=VMEM_LIMIT
        ),
    )(
        mx2, in2, ct, w_in_two, w_out_two, kernel_two, mx1, w_in_one, w_out_one, kernel_one,
    )
    scale = 1.0 / 16.0
    return out, gin.astype(F32) * scale, gout.astype(F32) * scale, gk * scale


def solution(mesh):
    finer = Mesh(mesh.devices.reshape(2, 4, 2, 4, 2), AXES)
    grid = P(DP, SPACE, None, None)
    return jax.shard_map(
        step,
        mesh=finer,
        in_specs=(grid, grid, grid, P(), P(), P(), grid, P(), P(), P()),
        out_specs=(grid, P(DP, None), P(DP, None), P()),
        check_vma=False,
    )
```
